8 devices in a mesh: dp: 1 (over z), sp2: 2 (over y), sp: 4 (over x, core).
Axes of the slice: x: 2, y: 2, z: 1, core: 2. Of those that a mesh axis runs over, the one named last changes fastest.
Arguments:
- x: bfloat16 [32, 32, 256, 128], P('dp', 'sp', 'sp2')
- w_a: bfloat16 [3, 3, 3, 128, 128], replicated
- bn_a: float32 [3, 2, 128], replicated
- w_down: bfloat16 [3, 3, 128, 256], replicated
- bn_down: float32 [2, 256], replicated
- w_b: bfloat16 [2, 3, 3, 256, 256], replicated
- bn_b: float32 [2, 2, 256], replicated
Outputs:
- output: bfloat16 [32, 16, 128, 256], P('dp', 'sp', 'sp2')
All inputs are finite; a program needn't handle non-finite values.
Results may differ from the reference program's by a relative error of at most 0.00764817.
Values are sent between devices in bfloat16 or wider.
A program may use at most 1 GiB of HBM per device.

```python
import jax
import jax.numpy as jnp
from jax import lax

IMAGES = 32
IMG_HEIGHT = 32
IMG_WIDTH = 256
CHAN_A = 128
CHAN_B = 256
LAYERS_A = 3
LAYERS_B = 2

CONV_DIMS = ("NHWC", "HWIO", "NHWC")
SAME_PADS = ((1, 1), (1, 1))
DOWN_PADS = ((0, 1), (0, 1))


def norm_pairs(pair_key, lead_shape, num_chan):
    gain_key, shift_key = jax.random.split(pair_key)
    gains = 1.0 + 0.3 * jax.random.normal(gain_key, lead_shape + (1, num_chan), jnp.float32)
    shifts = 0.5 * jax.random.normal(shift_key, lead_shape + (1, num_chan), jnp.float32)
    return jnp.concatenate([gains, shifts], axis=-2)


def conv_weights(w_key, lead_shape, chan_in, chan_out):
    raw_w = jax.random.normal(w_key, lead_shape + (3, 3, chan_in, chan_out), jnp.float32)
    return (raw_w * (9 * chan_in) ** -0.5).astype(jnp.bfloat16)


def setup_inputs(seed: int = 0, part: int = 0) -> dict:
    sub_keys = jax.random.split(jax.random.key(seed), 7)
    img_keys = jax.random.split(jax.random.fold_in(sub_keys[0], part), 3)
    noise = jax.random.normal(img_keys[0], (IMAGES, IMG_HEIGHT, IMG_WIDTH, CHAN_A), jnp.float32)
    row_amp = jax.random.normal(img_keys[1], (IMAGES, 1, 1, CHAN_A), jnp.float32)
    col_amp = jax.random.normal(img_keys[2], (IMAGES, 1, 1, CHAN_A), jnp.float32)
    row_pos = (2.0 * (jnp.arange(IMG_HEIGHT, dtype=jnp.float32) + 0.5) / IMG_HEIGHT - 1.0).reshape(1, IMG_HEIGHT, 1, 1)
    col_pos = (2.0 * (jnp.arange(IMG_WIDTH, dtype=jnp.float32) + 0.5) / IMG_WIDTH - 1.0).reshape(1, 1, IMG_WIDTH, 1)
    images = (noise + 1.5 * row_amp * row_pos + col_amp * col_pos).astype(jnp.bfloat16)
    return {
        "x": images,
        "w_a": conv_weights(sub_keys[1], (LAYERS_A,), CHAN_A, CHAN_A),
        "bn_a": norm_pairs(sub_keys[2], (LAYERS_A,), CHAN_A),
        "w_down": conv_weights(sub_keys[3], (), CHAN_A, CHAN_B),
        "bn_down": norm_pairs(sub_keys[4], (), CHAN_B),
        "w_b": conv_weights(sub_keys[5], (LAYERS_B,), CHAN_B, CHAN_B),
        "bn_b": norm_pairs(sub_keys[6], (LAYERS_B,), CHAN_B),
    }


def conv_bn(act_in, weight, norm_pair, stride, pad_pairs):
    pre_norm = lax.conv_general_dilated(act_in.astype(jnp.float32), weight.astype(jnp.float32), (stride, stride), pad_pairs, dimension_numbers=CONV_DIMS)
    num_pos = pre_norm.shape[0] * pre_norm.shape[1] * pre_norm.shape[2]
    mean_val = jnp.sum(pre_norm, axis=(0, 1, 2)) / num_pos
    var_val = jnp.sum(pre_norm * pre_norm, axis=(0, 1, 2)) / num_pos - mean_val * mean_val
    normed = norm_pair[0] * (pre_norm - mean_val) * lax.rsqrt(var_val + 1e-5) + norm_pair[1]
    return jnp.maximum(normed, 0.0).astype(jnp.bfloat16)


def reference(x, w_a, bn_a, w_down, bn_down, w_b, bn_b):
    def stage_step(carry_act, layer_in):
        return conv_bn(carry_act, layer_in[0], layer_in[1], 1, SAME_PADS), None

    act_out, scan_rest = lax.scan(stage_step, x, (w_a, bn_a))
    act_out = conv_bn(act_out, w_down, bn_down, 2, DOWN_PADS)
    act_out, scan_rest = lax.scan(stage_step, act_out, (w_b, bn_b))
    return act_out
```

```python
import functools

import jax
import jax.numpy as jnp
from jax import lax
from jax.experimental import pallas as pl
from jax.experimental.pallas import tpu as pltpu
from jax.sharding import PartitionSpec as P

EPS = 1e-5
NQ = 4
F32 = jnp.float32
BF16 = jnp.bfloat16


def stack_kernel(dims, x_hbm, wa_ref, bna_ref, wd_ref, bnd_ref, wb_ref, bnb_ref, y_ref,
                 xv, act, actb, z, stg, wp, wdp, cbuf_a, cbuf_b, stat,
                 x_sem, row_send, row_recv, misc_send, misc_recv, st_send, st_recv):
    imgs, rows, cols, ca, cb, la, lb, rows_n, cols_n = dims
    n_dev = rows_n * cols_n
    pairs = cols // 2
    rows_b, cols_b = rows // 2, cols // 2
    sp, sp2 = lax.axis_index("sp"), lax.axis_index("sp2")
    me = sp2 * rows_n + sp
    odd = sp % 2
    has_up, has_down = sp > 0, sp < rows_n - 1
    has = {0: has_up, 1: has_down}
    at_left = sp2 == 0

    def x_copy(r):
        return pltpu.make_async_copy(x_hbm.at[:, r], xv.at[:, r], x_sem.at[r])

    slow_row = odd * (rows - 1)
    fast_row = (rows - 1) - slow_row
    x_copy(slow_row).start()
    x_copy(fast_row).start()
    for r in range(1, rows - 1):
        x_copy(r).start()

    act[0] = jnp.zeros((cols + 2, imgs, ca), BF16)
    act[rows + 1] = jnp.zeros((cols + 2, imgs, ca), BF16)
    actb[0] = jnp.zeros((cols_b + 2, imgs, cb), BF16)
    actb[rows_b + 1] = jnp.zeros((cols_b + 2, imgs, cb), BF16)
    for r in range(1, rows + 1):
        for c in (0, cols + 1):
            act[r, c] = jnp.zeros((imgs, ca), BF16)
    for r in range(1, rows_b + 1):
        for c in (0, cols_b + 1):
            actb[r, c] = jnp.zeros((imgs, cb), BF16)

    barrier = pltpu.get_barrier_semaphore()

    def peer(d):
        q = (me + d) % n_dev
        return {"sp2": q // rows_n, "sp": q % rows_n}

    for d in range(1, n_dev):
        pl.semaphore_signal(barrier, inc=1, device_id=peer(d), device_id_type=pl.DeviceIdType.MESH)
    pl.semaphore_wait(barrier, n_dev - 1)

    def remote(src, dst, ssem, rsem, dev):
        return pltpu.make_async_remote_copy(src_ref=src, dst_ref=dst, send_sem=ssem, recv_sem=rsem,
                                            device_id=dev, device_id_type=pl.DeviceIdType.MESH)

    def vert(side):
        return {"sp": sp - 1 if side == 0 else sp + 1, "sp2": sp2}

    def diag(side):
        return {"sp": sp - 1 if side == 0 else sp + 1, "sp2": 1 - sp2}

    lateral = {"sp": sp, "sp2": 1 - sp2}

    def halo(buf, n_r, n_c):
        width = n_c // NQ
        edge_c = jnp.where(at_left, n_c, 1)
        halo_c = jnp.where(at_left, 0, n_c + 1)
        mine = (1, n_r)
        theirs = (n_r + 1, 0)

        def row_piece(side, q):
            cut = pl.ds(1 + q * width, width)
            return remote(buf.at[mine[side], cut], buf.at[theirs[side], cut], row_send.at[side, q],
                          row_recv.at[1 - side, q], vert(side))

        def corner(side):
            return remote(buf.at[mine[side], edge_c], buf.at[theirs[side], halo_c], misc_send.at[side],
                          misc_recv.at[1 - side], diag(side))

        def side_col(src):
            return remote(src, buf.at[pl.ds(1, n_r), halo_c], misc_send.at[2], misc_recv.at[2], lateral)

        my_halo_c = jnp.where(at_left, n_c + 1, 0)
        lands = (0, n_r + 1)

        def row_landing(side, q):
            cut = pl.ds(1 + q * width, width)
            return remote(buf.at[mine[side], cut], buf.at[lands[side], cut], row_send.at[side, q],
                          row_recv.at[side, q], vert(side))

        def corner_landing(side):
            return remote(buf.at[mine[side], edge_c], buf.at[lands[side], my_halo_c], misc_send.at[side],
                          misc_recv.at[side], diag(side))

        def side_landing(src):
            return remote(src, buf.at[pl.ds(1, n_r), my_halo_c], misc_send.at[2], misc_recv.at[2], lateral)

        return row_piece, corner, side_col, row_landing, corner_landing, side_landing

    def by_side(side_pred, fn):
        for side in (0, 1):
            pl.when(jnp.logical_and(side_pred(side), has[side]))(functools.partial(fn, side))

    is_slow = lambda side: odd == side
    is_fast = lambda side: odd != side

    def send_row(h, pred):
        def go(side):
            for q in range(NQ):
                h[0](side, q).start()
            h[1](side).start()
        by_side(pred, go)

    def wait_row(h, pred):
        def go(side):
            for q in range(NQ):
                h[3](side, q).wait_recv()
            h[4](side).wait_recv()
        by_side(pred, go)

    def drain_row(h, pred):
        def go(side):
            for q in range(NQ):
                h[0](side, q).wait_send()
            h[1](side).wait_send()
        by_side(pred, go)

    def all_sum(layer, s1, s2, fold):
        s1 = jnp.sum(s1, axis=0, keepdims=True)
        s2 = jnp.sum(s2, axis=0, keepdims=True)
        both = jnp.concatenate([s1, s2], axis=0)
        if fold:
            half = both[:, :ca] + both[:, ca:]
            both = jnp.concatenate([half, half], axis=1)
        stat[layer, me] = both
        sends = [remote(stat.at[layer, me], stat.at[layer, me], st_send.at[layer, d], st_recv.at[layer, d], peer(d))
                 for d in range(1, n_dev)]
        for s in sends:
            s.start()
        for d in range(1, n_dev):
            src = (me + n_dev - d) % n_dev
            remote(stat.at[layer, src], stat.at[layer, src], st_send.at[layer, d], st_recv.at[layer, d], peer(d)).wait_recv()
        for s in sends:
            s.wait_send()
        total = stat[layer, 0]
        for k in range(1, n_dev):
            total = total + stat[layer, k]
        return total

    def affine(total, num, gamma, beta):
        mean = total[0:1] / num
        var = total[1:2] / num - mean * mean
        return mean, gamma * lax.rsqrt(var + EPS), beta

    def load_x_row(r):
        x_copy(r).wait()

        def blk(c, carry):
            c0 = pl.multiple_of(c * 16, 16)
            for i in range(imgs):
                stg[pl.ds(i * 17, 16), :] = xv[i, r, pl.ds(c0, 16), :].astype(F32)
            for k in range(16):
                act[r + 1, 1 + c0 + k] = stg[pl.ds(k, imgs, stride=17), :].astype(BF16)
            return carry

        lax.fori_loop(0, cols // 16, blk, 0)

    def apply_bn(zz, aff):
        mean, scale, beta = aff
        return jnp.maximum((zz - mean) * scale + beta, 0.0).astype(BF16)

    JN = 8

    def norm_row_a(r, aff):
        def blk(c, carry):
            zz = z[r, pl.ds(pl.multiple_of(c * (JN * imgs), JN * imgs), JN * imgs), :]
            y = apply_bn(zz, aff).reshape(JN, imgs, 2 * ca)
            y = jnp.stack([y[:, :, :ca], y[:, :, ca:]], axis=1).reshape(2 * JN, imgs, ca)
            act[r + 1, pl.ds(1 + c * (2 * JN), 2 * JN)] = y
            return carry
        lax.fori_loop(0, pairs // JN, blk, 0)

    def norm_row_b(r, aff):
        def blk(c, carry):
            zz = z[r, pl.ds(pl.multiple_of(c * (JN * imgs), JN * imgs), JN * imgs), :]
            actb[r + 1, pl.ds(1 + c * JN, JN)] = apply_bn(zz, aff).reshape(JN, imgs, cb)
            return carry
        lax.fori_loop(0, cols_b // JN, blk, 0)

    def norm_col_a(aff):
        p = jnp.where(at_left, pairs - 1, 0)
        for r in range(rows):
            y = apply_bn(z[r, pl.ds(pl.multiple_of(p * imgs, imgs), imgs), :], aff)
            cbuf_a[r] = jnp.where(at_left, y[:, ca:], y[:, :ca])

    def norm_col_b(aff):
        p = jnp.where(at_left, cols_b - 1, 0)
        for r in range(rows_b):
            cbuf_b[r] = apply_bn(z[r, pl.ds(pl.multiple_of(p * imgs, imgs), imgs), :], aff)

    def put(r, c0, n_c, acc, s):
        z[r, c0 * imgs:(c0 + n_c) * imgs, :] = acc
        a3 = acc.reshape(n_c * imgs // 8, 8, acc.shape[-1])
        return s[0] + jnp.sum(a3, axis=0), s[1] + jnp.sum(a3 * a3, axis=0)

    JA = 16

    def conv_row_a(layer, r, s):
        for j0 in range(0, pairs, JA):
            parts = []
            for dy in range(3):
                v = act[r + dy, 2 * j0:2 * j0 + 2 * JA + 2].reshape(JA + 1, 2, imgs, ca)
                for c in range(4):
                    parts.append(v[c // 2:c // 2 + JA, c % 2].reshape(JA * imgs, ca))
            acc = jnp.dot(jnp.concatenate(parts, axis=1), wp[layer], preferred_element_type=F32)
            s = put(r, j0, JA, acc, s)
        return s

    JD = 16

    def conv_row_d(i, s):
        for c0 in range(0, cols_b, JD):
            first, last = [], []
            for dy in range(3):
                v = act[2 * i + dy + 1, 2 * c0 + 1:2 * c0 + 2 * JD + 2]
                a = v[:2 * JD].reshape(JD, 2, imgs, ca)
                b = v[1:].reshape(JD, 2, imgs, ca)
                first += [a[:, 0].reshape(JD * imgs, ca), a[:, 1].reshape(JD * imgs, ca)]
                last.append(b[:, 1].reshape(JD * imgs, ca))
            acc = jnp.dot(jnp.concatenate(first + last, axis=1), wdp[...], preferred_element_type=F32)
            s = put(i, c0, JD, acc, s)
        return s

    JB = 16

    def conv_row_b(layer, r, s):
        for c0 in range(0, cols_b, JB):
            parts = []
            for dy in range(3):
                for dx in range(3):
                    parts.append(actb[r + dy, c0 + dx:c0 + dx + JB].reshape(JB * imgs, cb))
            acc = jnp.dot(jnp.concatenate(parts, axis=1), wb_ref[layer], preferred_element_type=F32)
            s = put(r, c0, JB, acc, s)
        return s

    zero_stat = lambda: (jnp.zeros((8, 256), F32), jnp.zeros((8, 256), F32))

    for layer in range(la):
        for dy in range(3):
            for c in range(4):
                k0 = (dy * 4 + c) * ca
                zero = jnp.zeros((ca, ca), BF16)
                wp[layer, k0:k0 + ca, :ca] = wa_ref[layer, dy, c] if c < 3 else zero
                wp[layer, k0:k0 + ca, ca:] = wa_ref[layer, dy, c - 1] if c > 0 else zero
    order = [(dy, dx) for dy in range(3) for dx in range(2)] + [(dy, 2) for dy in range(3)]
    for k, (dy, dx) in enumerate(order):
        wdp[k * ca:(k + 1) * ca, :] = wd_ref[dy, dx]

    num_a = float(imgs * rows * cols * n_dev)
    num_b = float(imgs * rows_b * cols_b * n_dev)

    def dup(v):
        return jnp.concatenate([v, v], axis=1)

    ha = halo(act, rows, cols)
    aff = None
    for layer in range(la):
        if layer == 0:
            load_x_row(slow_row)
            send_row(ha, is_slow)
            load_x_row(fast_row)
            send_row(ha, is_fast)
            lax.fori_loop(1, rows - 1, lambda r, c: (load_x_row(r), c)[1], 0)
            edge_c = jnp.where(at_left, cols, 1)
            col_src = act.at[pl.ds(1, rows), edge_c]
            ha[2](col_src).start()
        else:
            norm_row_a(slow_row, aff)
            norm_col_a(aff)
            send_row(ha, is_slow)
            norm_row_a(fast_row, aff)
            send_row(ha, is_fast)
            col_src = cbuf_a
            ha[2](col_src).start()
            lax.fori_loop(1, rows - 1, lambda r, c: (norm_row_a(r, aff), c)[1], 0)
        ha[5](col_src).wait_recv()

        def step(k, s):
            @pl.when(k == rows - 1)
            def _():
                wait_row(ha, is_fast)

            @pl.when(k == rows)
            def _():
                wait_row(ha, is_slow)

            r = jnp.where(k == rows - 1, fast_row, jnp.where(k == rows, slow_row, k))
            return conv_row_a(layer, r, s)

        s1, s2 = lax.fori_loop(1, rows + 1, step, zero_stat())
        total = all_sum(layer, s1, s2, True)
        drain_row(ha, is_slow)
        drain_row(ha, is_fast)
        ha[2](col_src).wait_send()
        aff = affine(total, num_a, dup(bna_ref[layer, 0:1]), dup(bna_ref[layer, 1:2]))

    norm_row_a(0, aff)
    norm_col_a(aff)

    @pl.when(has_up)
    def _():
        for q in range(NQ):
            ha[0](0, q).start()

        @pl.when(sp2 == 1)
        def _():
            ha[1](0).start()

    @pl.when(sp2 == 1)
    def _():
        ha[2](cbuf_a).start()

    lax.fori_loop(1, rows, lambda r, c: (norm_row_a(r, aff), c)[1], 0)

    @pl.when(sp2 == 0)
    def _():
        ha[5](cbuf_a).wait_recv()

    def step_d(i, s):
        @pl.when(jnp.logical_and(i == rows_b - 1, has_down))
        def _():
            for q in range(NQ):
                ha[3](1, q).wait_recv()

            @pl.when(sp2 == 0)
            def _():
                ha[4](1).wait_recv()

        return conv_row_d(i, s)

    s1, s2 = lax.fori_loop(0, rows_b, step_d, zero_stat())
    total = all_sum(la, s1, s2, False)

    @pl.when(has_up)
    def _():
        for q in range(NQ):
            ha[0](0, q).wait_send()

        @pl.when(sp2 == 1)
        def _():
            ha[1](0).wait_send()

    @pl.when(sp2 == 1)
    def _():
        ha[2](cbuf_a).wait_send()

    aff = affine(total, num_b, bnd_ref[0:1], bnd_ref[1:2])

    hb = halo(actb, rows_b, cols_b)
    slow_b = odd * (rows_b - 1)
    fast_b = (rows_b - 1) - slow_b
    for layer in range(lb):
        norm_row_b(slow_b, aff)
        norm_col_b(aff)
        send_row(hb, is_slow)
        norm_row_b(fast_b, aff)
        send_row(hb, is_fast)
        hb[2](cbuf_b).start()
        lax.fori_loop(1, rows_b - 1, lambda r, c: (norm_row_b(r, aff), c)[1], 0)
        hb[5](cbuf_b).wait_recv()

        def step_b(k, s):
            @pl.when(k == rows_b - 1)
            def _():
                wait_row(hb, is_fast)

            @pl.when(k == rows_b)
            def _():
                wait_row(hb, is_slow)

            r = jnp.where(k == rows_b - 1, fast_b, jnp.where(k == rows_b, slow_b, k))
            return conv_row_b(layer, r, s)

        s1, s2 = lax.fori_loop(1, rows_b + 1, step_b, zero_stat())
        total = all_sum(la + 1 + layer, s1, s2, False)
        drain_row(hb, is_slow)
        drain_row(hb, is_fast)
        hb[2](cbuf_b).wait_send()
        aff = affine(total, num_b, bnb_ref[layer, 0:1], bnb_ref[layer, 1:2])

    def final_row(r, carry):
        def blk(c, carry):
            zz = z[r, pl.ds(pl.multiple_of(c * (JN * imgs), JN * imgs), JN * imgs), :]
            y_ref[r, pl.ds(c * JN, JN)] = apply_bn(zz, aff).reshape(JN, imgs, cb)
            return carry
        return lax.fori_loop(0, cols_b // JN, blk, carry)

    lax.fori_loop(0, rows_b, final_row, 0)


def solution(mesh):
    rows_n, cols_n = mesh.shape["sp"], mesh.shape["sp2"]

    def per_device(x, w_a, bn_a, w_down, bn_down, w_b, bn_b):
        imgs, rows, cols, ca = x.shape
        cb = w_down.shape[-1]
        la, lb = w_a.shape[0], w_b.shape[0]
        rows_b, cols_b = rows // 2, cols // 2
        dims = (imgs, rows, cols, ca, cb, la, lb, rows_n, cols_n)
        n_dev = rows_n * cols_n
        layers = la + 1 + lb
        vm = pl.BlockSpec(memory_space=pltpu.VMEM)
        dma = pltpu.SemaphoreType.DMA
        y = pl.pallas_call(
            functools.partial(stack_kernel, dims),
            out_shape=jax.ShapeDtypeStruct((rows_b, cols_b, imgs, cb), BF16),
            in_specs=[pl.BlockSpec(memory_space=pl.ANY)] + [vm] * 6,
            out_specs=vm,
            scratch_shapes=[
                pltpu.VMEM((imgs, rows, cols, ca), BF16),
                pltpu.VMEM((rows + 2, cols + 2, imgs, ca), BF16),
                pltpu.VMEM((rows_b + 2, cols_b + 2, imgs, cb), BF16),
                pltpu.VMEM((rows, cols // 2 * imgs, 2 * ca), F32),
                pltpu.VMEM((imgs * 17 + 16, ca), F32),
                pltpu.VMEM((la, 12 * ca, 2 * ca), BF16),
                pltpu.VMEM((9 * ca, cb), BF16),
                pltpu.VMEM((rows, imgs, ca), BF16),
                pltpu.VMEM((rows_b, imgs, cb), BF16),
                pltpu.VMEM((layers, n_dev, 2, 256), F32),
                dma((rows,)),
                dma((2, NQ)), dma((2, NQ)), dma((3,)), dma((3,)), dma((layers, n_dev)), dma((layers, n_dev)),
            ],
            compiler_params=pltpu.CompilerParams(
                collective_id=0, has_side_effects=True, vmem_limit_bytes=66_000_000),
            name="stack",
        )(x, w_a, bn_a, w_down, bn_down, w_b.reshape(lb, 9 * cb, cb), bn_b)
        return y.transpose(2, 0, 1, 3)

    tile_spec = P("dp", "sp", "sp2", None)
    return jax.shard_map(per_device, mesh=mesh, in_specs=(tile_spec, P(), P(), P(), P(), P(), P()),
                         out_specs=tile_spec, check_vma=False)
```

```python
import functools

import jax
import jax.numpy as jnp
from jax import lax
from jax.experimental import pallas as pl
from jax.experimental.pallas import tpu as pltpu
from jax.sharding import PartitionSpec as P

EPS = 1e-5
NQ = 4
F32 = jnp.float32
BF16 = jnp.bfloat16


def stack_kernel(dims, x_hbm, wa_ref, bna_ref, wd_ref, bnd_ref, wb_ref, bnb_ref, y_ref,
                 xv, act, actb, z, stg, wp, wdp, wbv, cbuf_a, cbuf_b, stat,
                 x_sem, w_sem, row_send, row_recv, misc_send, misc_recv, st_send, st_recv):
    imgs, rows, cols, ca, cb, la, lb, rows_n, cols_n = dims
    n_dev = rows_n * cols_n
    pairs = cols // 2
    rows_b, cols_b = rows // 2, cols // 2
    sp, sp2 = lax.axis_index("sp"), lax.axis_index("sp2")
    me = sp2 * rows_n + sp
    odd = sp % 2
    has_up, has_down = sp > 0, sp < rows_n - 1
    has = {0: has_up, 1: has_down}
    at_left = sp2 == 0

    def x_copy(r):
        return pltpu.make_async_copy(x_hbm.at[:, r], xv.at[:, r], x_sem.at[r])

    slow_row = odd * (rows - 1)
    fast_row = (rows - 1) - slow_row
    x_copy(slow_row).start()
    x_copy(fast_row).start()
    for r in range(1, rows - 1):
        x_copy(r).start()

    order = [(dy, dx) for dy in range(3) for dx in range(2)] + [(dy, 2) for dy in range(3)]
    w_copies = [pltpu.make_async_copy(wd_ref.at[dy, dx], wdp.at[pl.ds(k * ca, ca)], w_sem.at[k])
                for k, (dy, dx) in enumerate(order)]
    w_copies.append(pltpu.make_async_copy(wb_ref, wbv, w_sem.at[9]))
    for c in w_copies:
        c.start()

    act[0] = jnp.zeros((cols + 2, imgs, ca), BF16)
    act[rows + 1] = jnp.zeros((cols + 2, imgs, ca), BF16)
    actb[0] = jnp.zeros((cols_b + 2, imgs, cb), BF16)
    actb[rows_b + 1] = jnp.zeros((cols_b + 2, imgs, cb), BF16)
    for r in range(1, rows + 1):
        for c in (0, cols + 1):
            act[r, c] = jnp.zeros((imgs, ca), BF16)
    for r in range(1, rows_b + 1):
        for c in (0, cols_b + 1):
            actb[r, c] = jnp.zeros((imgs, cb), BF16)

    barrier = pltpu.get_barrier_semaphore()

    def peer(d):
        q = (me + d) % n_dev
        return {"sp2": q // rows_n, "sp": q % rows_n}

    for d in range(1, n_dev):
        pl.semaphore_signal(barrier, inc=1, device_id=peer(d), device_id_type=pl.DeviceIdType.MESH)
    pl.semaphore_wait(barrier, n_dev - 1)

    def remote(src, dst, ssem, rsem, dev):
        return pltpu.make_async_remote_copy(src_ref=src, dst_ref=dst, send_sem=ssem, recv_sem=rsem,
                                            device_id=dev, device_id_type=pl.DeviceIdType.MESH)

    def vert(side):
        return {"sp": sp - 1 if side == 0 else sp + 1, "sp2": sp2}

    def diag(side):
        return {"sp": sp - 1 if side == 0 else sp + 1, "sp2": 1 - sp2}

    lateral = {"sp": sp, "sp2": 1 - sp2}

    def halo(buf, cbuf, n_r, n_c):
        ends = [(q + 1) * n_c // NQ + 2 for q in range(NQ - 1)] + [n_c + 1]
        cuts = [pl.ds(a, b - a) for a, b in zip([1] + ends[:-1], ends)]
        halo_c = jnp.where(at_left, 0, n_c + 1)
        mine, edge_r = (1, n_r), (0, n_r - 1)
        theirs = (n_r + 1, 0)

        def row_piece(side, q):
            cut = cuts[q]
            return remote(buf.at[mine[side], cut], buf.at[theirs[side], cut], row_send.at[side, q],
                          row_recv.at[1 - side, q], vert(side))

        def corner(side):
            return remote(cbuf.at[edge_r[side]], buf.at[theirs[side], halo_c], misc_send.at[side],
                          misc_recv.at[1 - side], diag(side))

        def side_col(src):
            return remote(src, buf.at[pl.ds(1, n_r), halo_c], misc_send.at[2], misc_recv.at[2], lateral)

        my_halo_c = jnp.where(at_left, n_c + 1, 0)
        lands = (0, n_r + 1)

        def row_landing(side, q):
            cut = cuts[q]
            return remote(buf.at[mine[side], cut], buf.at[lands[side], cut], row_send.at[side, q],
                          row_recv.at[side, q], vert(side))

        def corner_landing(side):
            return remote(cbuf.at[edge_r[side]], buf.at[lands[side], my_halo_c], misc_send.at[side],
                          misc_recv.at[side], diag(side))

        def side_landing(src):
            return remote(src, buf.at[pl.ds(1, n_r), my_halo_c], misc_send.at[2], misc_recv.at[2], lateral)

        return row_piece, corner, side_col, row_landing, corner_landing, side_landing

    def by_side(side_pred, fn):
        for side in (0, 1):
            pl.when(jnp.logical_and(side_pred(side), has[side]))(functools.partial(fn, side))

    is_slow = lambda side: odd == side
    is_fast = lambda side: odd != side

    def send_corner(h, pred):
        by_side(pred, lambda side: h[1](side).start())

    def produce_row(h, pred, make, tail=None):
        make(0)
        for q in range(1, NQ):
            make(q)
            by_side(pred, lambda side, q=q: h[0](side, q - 1).start())
        if tail is not None:
            tail()
        by_side(pred, lambda side: h[0](side, NQ - 1).start())

    def wait_row(h, pred, part, n_parts):
        def go(side):
            if part == 0:
                h[4](side).wait_recv()
            for q in range(part * NQ // n_parts, (part + 1) * NQ // n_parts):
                h[3](side, q).wait_recv()
        by_side(pred, go)

    def drain_row(h, pred):
        def go(side):
            for q in range(NQ):
                h[0](side, q).wait_send()
            h[1](side).wait_send()
        by_side(pred, go)

    def all_sum(layer, s1, s2, fold):
        s1 = jnp.sum(s1, axis=0, keepdims=True)
        s2 = jnp.sum(s2, axis=0, keepdims=True)
        both = jnp.concatenate([s1, s2], axis=0)
        if fold:
            half = both[:, :ca] + both[:, ca:]
            both = jnp.concatenate([half, half], axis=1)
        stat[layer, me] = both
        sends = [remote(stat.at[layer, me], stat.at[layer, me], st_send.at[layer, d], st_recv.at[layer, d], peer(d))
                 for d in range(1, n_dev)]
        for s in sends:
            s.start()
        for d in range(1, n_dev):
            src = (me + n_dev - d) % n_dev
            remote(stat.at[layer, src], stat.at[layer, src], st_send.at[layer, d], st_recv.at[layer, d], peer(d)).wait_recv()
        for s in sends:
            s.wait_send()
        total = stat[layer, 0]
        for k in range(1, n_dev):
            total = total + stat[layer, k]
        return total

    def affine(total, num, gamma, beta):
        mean = total[0:1] / num
        var = total[1:2] / num - mean * mean
        return mean, gamma * lax.rsqrt(var + EPS), beta

    def group(n, q):
        return (0, n) if q is None else (q * n // NQ, (q + 1) * n // NQ)

    def load_x_row(r, q=None):
        if q is None:
            x_copy(r).wait()
        load_x(r, *group(cols // 16, q))

    def load_x(r, lo, hi):
        def blk(c, carry):
            c0 = pl.multiple_of(c * 16, 16)
            for i in range(imgs):
                stg[0, pl.ds(i * 17, 16), :] = xv[i, r, pl.ds(c0, 16), :].astype(F32)
            for k in range(16):
                act[r + 1, 1 + c0 + k] = stg[0, pl.ds(k, imgs, stride=17), :].astype(BF16)
            return carry

        lax.fori_loop(lo, hi, blk, 0)

    def apply_bn(zz, aff):
        mean, scale, beta = aff
        return jnp.maximum((zz - mean) * scale + beta, 0.0)

    JN = 8

    def norm_row_a(r, aff, q=None):
        def blk(c, carry):
            zz = z[r, pl.ds(pl.multiple_of(c * (JN * imgs), JN * imgs), JN * imgs), :]
            y = apply_bn(zz, aff).astype(BF16).reshape(JN, imgs, 2 * ca)
            y = jnp.stack([y[:, :, :ca], y[:, :, ca:]], axis=1).reshape(2 * JN, imgs, ca)
            act[r + 1, pl.ds(1 + c * (2 * JN), 2 * JN)] = y
            return carry
        lax.fori_loop(*group(pairs // JN, q), blk, 0)

    def norm_row_b(r, aff, q=None):
        def blk(c, carry):
            zz = z[r, pl.ds(pl.multiple_of(c * (JN * imgs), JN * imgs), JN * imgs), :]
            actb[r + 1, pl.ds(1 + c * JN, JN)] = apply_bn(zz, aff).astype(BF16).reshape(JN, imgs, cb)
            return carry
        lax.fori_loop(*group(cols_b // JN, q), blk, 0)

    def norm_col_a(aff):
        p = jnp.where(at_left, pairs - 1, 0)
        for r in range(rows):
            y = apply_bn(z[r, pl.ds(pl.multiple_of(p * imgs, imgs), imgs), :], aff).astype(BF16)
            cbuf_a[r] = jnp.where(at_left, y[:, ca:], y[:, :ca])

    def norm_col_b(aff):
        p = jnp.where(at_left, cols_b - 1, 0)
        for r in range(rows_b):
            cbuf_b[r] = apply_bn(z[r, pl.ds(pl.multiple_of(p * imgs, imgs), imgs), :], aff).astype(BF16)

    def put(r, c0, n_c, acc, s):
        z[r, pl.ds(pl.multiple_of(c0 * imgs, 8 * imgs), n_c * imgs), :] = acc
        a3 = acc.reshape(n_c * imgs // 8, 8, acc.shape[-1])
        return s[0] + jnp.sum(a3, axis=0), s[1] + jnp.sum(a3 * a3, axis=0)

    JC = 16
    NC_A, NC_B = pairs // JC, cols_b // JC

    def conv_a(layer, r, j, s):
        parts = []
        for dy in range(3):
            v = act[r + dy, pl.ds(2 * JC * j, 2 * JC + 2)].reshape(JC + 1, 2, imgs, ca)
            for c in range(4):
                parts.append(v[c // 2:c // 2 + JC, c % 2].reshape(JC * imgs, ca))
        acc = jnp.dot(jnp.concatenate(parts, axis=1), wp[layer], preferred_element_type=F32)
        return put(r, JC * j, JC, acc, s)

    def conv_d(i, j, s):
        first, last = [], []
        for dy in range(3):
            v = act[2 * i + dy + 1, pl.ds(2 * JC * j + 1, 2 * JC + 1)]
            a = v[:2 * JC].reshape(JC, 2, imgs, ca)
            b = v[1:].reshape(JC, 2, imgs, ca)
            first += [a[:, 0].reshape(JC * imgs, ca), a[:, 1].reshape(JC * imgs, ca)]
            last.append(b[:, 1].reshape(JC * imgs, ca))
        acc = jnp.dot(jnp.concatenate(first + last, axis=1), wdp[...], preferred_element_type=F32)
        return put(i, JC * j, JC, acc, s)

    def conv_b(layer, r, j, s):
        parts = []
        for dy in range(3):
            for dx in range(3):
                parts.append(actb[r + dy, pl.ds(JC * j + dx, JC)].reshape(JC * imgs, cb))
        acc = jnp.dot(jnp.concatenate(parts, axis=1), wbv[layer], preferred_element_type=F32)
        return put(r, JC * j, JC, acc, s)

    zero_stat = lambda: (jnp.zeros((8, 256), F32), jnp.zeros((8, 256), F32))

    for layer in range(la):
        for dy in range(3):
            for c in range(4):
                k0 = (dy * 4 + c) * ca
                zero = jnp.zeros((ca, ca), BF16)
                wp[layer, k0:k0 + ca, :ca] = wa_ref[layer, dy, c] if c < 3 else zero
                wp[layer, k0:k0 + ca, ca:] = wa_ref[layer, dy, c - 1] if c > 0 else zero

    num_a = float(imgs * rows * cols * n_dev)
    num_b = float(imgs * rows_b * cols_b * n_dev)

    def dup(v):
        return jnp.concatenate([v, v], axis=1)

    ha = halo(act, cbuf_a, rows, cols)
    PA, PB = 2, 4

    def layer_a(layer, aff):
        @pl.when(layer == 0)
        def _():
            edge_b = jnp.where(at_left, cols // 16 - 1, 0)
            edge_c = jnp.where(at_left, cols, 1)
            for row, pred in ((slow_row, is_slow), (fast_row, is_fast)):
                x_copy(row).wait()
                load_x(row, edge_b, edge_b + 1)
                cbuf_a[row] = act[row + 1, edge_c]
                send_corner(ha, pred)
                produce_row(ha, pred, functools.partial(load_x_row, row))

            def inner(r, c):
                load_x_row(r)
                return c
            lax.fori_loop(1, rows - 1, inner, 0)
            for r in range(1, rows - 1):
                cbuf_a[r] = act[r + 1, edge_c]
            ha[2](cbuf_a).start()

        @pl.when(layer > 0)
        def _():
            norm_col_a(aff)
            norm_row_a(slow_row, aff, 0)
            send_corner(ha, is_slow)
            ha[2](cbuf_a).start()
            send_corner(ha, is_fast)
            produce_row(ha, is_slow, lambda q: norm_row_a(slow_row, aff, q) if q else None)
            produce_row(ha, is_fast, lambda q: norm_row_a(fast_row, aff, q))

            def inner(r, c):
                norm_row_a(r, aff)
                return c
            lax.fori_loop(1, rows - 1, inner, 0)

        def step(it, s):
            pl.when(it == 1)(lambda: ha[5](cbuf_a).wait_recv())
            for r in range(1, rows - 1):
                for u in range(NC_A // 2):
                    mid = NC_A // 4 + u
                    outer = u if u < NC_A // 4 else NC_A // 2 + u
                    s = conv_a(layer, r, jnp.where(it == 0, mid, outer), s)
            return s

        s = lax.fori_loop(0, 2, step, zero_stat())
        wait_row(ha, is_fast, 0, 1)
        for j in range(NC_A):
            s = conv_a(layer, fast_row, j, s)
        for part in range(PA):
            wait_row(ha, is_slow, part, PA)
            for j in range(part * NC_A // PA, (part + 1) * NC_A // PA):
                s = conv_a(layer, slow_row, j, s)
        total = all_sum(layer, *s, True)
        drain_row(ha, is_slow)
        drain_row(ha, is_fast)
        ha[2](cbuf_a).wait_send()
        return affine(total, num_a, dup(bna_ref[layer, 0:1]), dup(bna_ref[layer, 1:2]))

    no_aff = tuple(jnp.zeros((1, 2 * ca), F32) for _ in range(3))
    aff = lax.fori_loop(0, la, layer_a, no_aff)

    norm_col_a(aff)
    norm_row_a(0, aff, 0)

    @pl.when(sp2 == 1)
    def _():
        pl.when(has_up)(lambda: ha[1](0).start())
        ha[2](cbuf_a).start()

    for q in range(1, NQ):
        norm_row_a(0, aff, q)
        pl.when(has_up)(lambda q=q: ha[0](0, q - 1).start())
    pl.when(has_up)(lambda: ha[0](0, NQ - 1).start())

    def inner_d(r, c):
        norm_row_a(r, aff)
        return c

    lax.fori_loop(1, rows, inner_d, 0)
    for c in w_copies:
        c.wait()

    s = zero_stat()
    for i in range(rows_b - 1):
        for j in range(NC_B - 1):
            s = conv_d(i, j, s)
    pl.when(sp2 == 0)(lambda: ha[5](cbuf_a).wait_recv())
    for i in range(rows_b - 1):
        s = conv_d(i, NC_B - 1, s)
    for part in range(PB):
        @pl.when(has_down)
        def _():
            if part == 0:
                pl.when(sp2 == 0)(lambda: ha[4](1).wait_recv())
            for q in range(part * NQ // PB, (part + 1) * NQ // PB):
                ha[3](1, q).wait_recv()
        for j in range(part * NC_B // PB, (part + 1) * NC_B // PB):
            s = conv_d(rows_b - 1, j, s)
    total = all_sum(la, *s, False)

    @pl.when(has_up)
    def _():
        for q in range(NQ):
            ha[0](0, q).wait_send()
        pl.when(sp2 == 1)(lambda: ha[1](0).wait_send())

    @pl.when(sp2 == 1)
    def _():
        ha[2](cbuf_a).wait_send()

    aff = affine(total, num_b, bnd_ref[0:1], bnd_ref[1:2])

    hb = halo(actb, cbuf_b, rows_b, cols_b)
    slow_b = odd * (rows_b - 1)
    fast_b = (rows_b - 1) - slow_b

    def layer_b(layer, aff):
        norm_col_b(aff)
        norm_row_b(slow_b, aff, 0)
        send_corner(hb, is_slow)
        hb[2](cbuf_b).start()
        send_corner(hb, is_fast)
        produce_row(hb, is_slow, lambda q: norm_row_b(slow_b, aff, q) if q else None)
        produce_row(hb, is_fast, lambda q: norm_row_b(fast_b, aff, q))

        def inner(r, c):
            norm_row_b(r, aff)
            return c
        lax.fori_loop(1, rows_b - 1, inner, 0)
        s = zero_stat()
        for r in range(1, rows_b - 1):
            for j in range(1, NC_B - 1):
                s = conv_b(layer, r, j, s)
        hb[5](cbuf_b).wait_recv()
        wait_row(hb, is_fast, 0, 1)
        for r in range(1, rows_b - 1):
            for j in (0, NC_B - 1):
                s = conv_b(layer, r, j, s)
        for j in range(NC_B):
            s = conv_b(layer, fast_b, j, s)
        for part in range(PB):
            wait_row(hb, is_slow, part, PB)
            for j in range(part * NC_B // PB, (part + 1) * NC_B // PB):
                s = conv_b(layer, slow_b, j, s)
        total = all_sum(la + 1 + layer, *s, False)
        drain_row(hb, is_slow)
        drain_row(hb, is_fast)
        hb[2](cbuf_b).wait_send()
        return affine(total, num_b, bnb_ref[layer, 0:1], bnb_ref[layer, 1:2])

    aff = lax.fori_loop(0, lb, layer_b, aff)

    def final_row(r, carry):
        def blk(c, carry):
            c0 = pl.multiple_of(c * 16, 16)
            for k in range(16):
                y = apply_bn(z[r, pl.ds(pl.multiple_of(c0 * imgs + k * imgs, imgs), imgs), :], aff)
                for h in range(2):
                    stg[h, pl.ds(k * 33, imgs), :] = y[:, h * 128:(h + 1) * 128]
            for i in range(imgs):
                for h in range(2):
                    y_ref[i, r, pl.ds(c0, 16), h * 128:(h + 1) * 128] = stg[h, pl.ds(i, 16, stride=33), :].astype(BF16)
            return carry
        return lax.fori_loop(0, cols_b // 16, blk, carry)

    lax.fori_loop(0, rows_b, final_row, 0)


def solution(mesh):
    rows_n, cols_n = mesh.shape["sp"], mesh.shape["sp2"]

    def per_device(x, w_a, bn_a, w_down, bn_down, w_b, bn_b):
        imgs, rows, cols, ca = x.shape
        cb = w_down.shape[-1]
        la, lb = w_a.shape[0], w_b.shape[0]
        rows_b, cols_b = rows // 2, cols // 2
        dims = (imgs, rows, cols, ca, cb, la, lb, rows_n, cols_n)
        n_dev = rows_n * cols_n
        layers = la + 1 + lb
        vm = pl.BlockSpec(memory_space=pltpu.VMEM)
        hbm = pl.BlockSpec(memory_space=pl.ANY)
        dma = pltpu.SemaphoreType.DMA
        return pl.pallas_call(
            functools.partial(stack_kernel, dims),
            out_shape=jax.ShapeDtypeStruct((imgs, rows_b, cols_b, cb), BF16),
            in_specs=[hbm, vm, vm, hbm, vm, hbm, vm],
            out_specs=vm,
            scratch_shapes=[
                pltpu.VMEM((imgs, rows, cols, ca), BF16),
                pltpu.VMEM((rows + 2, cols + 2, imgs, ca), BF16),
                pltpu.VMEM((rows_b + 2, cols_b + 2, imgs, cb), BF16),
                pltpu.VMEM((rows, cols // 2 * imgs, 2 * ca), F32),
                pltpu.VMEM((2, imgs * 17 + 16, 128), F32),
                pltpu.VMEM((la, 12 * ca, 2 * ca), BF16),
                pltpu.VMEM((9 * ca, cb), BF16),
                pltpu.VMEM((lb, 9 * cb, cb), BF16),
                pltpu.VMEM((rows, imgs, ca), BF16),
                pltpu.VMEM((rows_b, imgs, cb), BF16),
                pltpu.VMEM((layers, n_dev, 2, 256), F32),
                dma((rows,)), dma((10,)),
                dma((2, NQ)), dma((2, NQ)), dma((3,)), dma((3,)), dma((layers, n_dev)), dma((layers, n_dev)),
            ],
            compiler_params=pltpu.CompilerParams(
                collective_id=0, has_side_effects=True, vmem_limit_bytes=66_000_000),
            name="stack",
        )(x, w_a, bn_a, w_down, bn_down, w_b.reshape(lb, 9 * cb, cb), bn_b)

    tile_spec = P("dp", "sp", "sp2", None)
    return jax.shard_map(per_device, mesh=mesh, in_specs=(tile_spec, P(), P(), P(), P(), P(), P()),
                         out_specs=tile_spec, check_vma=False)
```

```python
import functools

import jax
import jax.numpy as jnp
from jax import lax
from jax.experimental import pallas as pl
from jax.experimental.pallas import tpu as pltpu
from jax.sharding import PartitionSpec as P

EPS = 1e-5
FRAC = (2, 4, 6, 7, 8)
NQ = len(FRAC)
F32 = jnp.float32
BF16 = jnp.bfloat16


def stack_kernel(dims, x_hbm, wa_hbm, bna_hbm, wd_ref, bnd_hbm, wb_ref, bnb_hbm, y_ref,
                 wa_ref, bna_ref, bnd_ref, bnb_ref, xv, act, actb, z, stg, wp, wdp, wbv, cbuf_a, cbuf_b, stat,
                 x_sem, w_sem, row_send, row_recv, misc_send, misc_recv, st_send, st_recv):
    imgs, rows, cols, ca, cb, la, lb, rows_n, cols_n = dims
    n_dev = rows_n * cols_n
    pairs = cols // 2
    rows_b, cols_b = rows // 2, cols // 2
    sp, sp2 = lax.axis_index("sp"), lax.axis_index("sp2")
    me = sp2 * rows_n + sp
    odd = sp % 2
    has_up, has_down = sp > 0, sp < rows_n - 1
    has = {0: has_up, 1: has_down}
    at_left = sp2 == 0

    def x_copy(r):
        return pltpu.make_async_copy(x_hbm.at[:, r], xv.at[:, r], x_sem.at[r])

    slow_row = odd * (rows - 1)
    fast_row = (rows - 1) - slow_row
    x_copy(slow_row).start()
    x_copy(fast_row).start()
    for r in range(1, rows - 1):
        x_copy(r).start()

    early = [pltpu.make_async_copy(a, b, w_sem.at[10 + k]) for k, (a, b) in enumerate(
        ((wa_hbm, wa_ref), (bna_hbm, bna_ref), (bnd_hbm, bnd_ref), (bnb_hbm, bnb_ref)))]
    for c in early:
        c.start()

    order = [(dy, dx) for dy in range(3) for dx in range(2)] + [(dy, 2) for dy in range(3)]
    w_copies = [pltpu.make_async_copy(wd_ref.at[dy, dx], wdp.at[pl.ds(k * ca, ca)], w_sem.at[k])
                for k, (dy, dx) in enumerate(order)]
    w_copies.append(pltpu.make_async_copy(wb_ref, wbv, w_sem.at[9]))
    for c in w_copies:
        c.start()

    act[0] = jnp.zeros((cols + 2, imgs, ca), BF16)
    act[rows + 1] = jnp.zeros((cols + 2, imgs, ca), BF16)
    actb[0] = jnp.zeros((cols_b + 2, imgs, cb), BF16)
    actb[rows_b + 1] = jnp.zeros((cols_b + 2, imgs, cb), BF16)
    for r in range(1, rows + 1):
        for c in (0, cols + 1):
            act[r, c] = jnp.zeros((imgs, ca), BF16)
    for r in range(1, rows_b + 1):
        for c in (0, cols_b + 1):
            actb[r, c] = jnp.zeros((imgs, cb), BF16)

    barrier = pltpu.get_barrier_semaphore()

    def peer(d):
        q = (me + d) % n_dev
        return {"sp2": q // rows_n, "sp": q % rows_n}

    for d in range(1, n_dev):
        pl.semaphore_signal(barrier, inc=1, device_id=peer(d), device_id_type=pl.DeviceIdType.MESH)
    pl.semaphore_wait(barrier, n_dev - 1)

    def remote(src, dst, ssem, rsem, dev):
        return pltpu.make_async_remote_copy(src_ref=src, dst_ref=dst, send_sem=ssem, recv_sem=rsem,
                                            device_id=dev, device_id_type=pl.DeviceIdType.MESH)

    def vert(side):
        return {"sp": sp - 1 if side == 0 else sp + 1, "sp2": sp2}

    def diag(side):
        return {"sp": sp - 1 if side == 0 else sp + 1, "sp2": 1 - sp2}

    lateral = {"sp": sp, "sp2": 1 - sp2}

    def halo(buf, cbuf, n_r, n_c):
        ends = [f * n_c // 8 + 2 for f in FRAC[:-1]] + [n_c + 1]
        cuts = [pl.ds(a, b - a) for a, b in zip([1] + ends[:-1], ends)]
        halo_c = jnp.where(at_left, 0, n_c + 1)
        mine, edge_r = (1, n_r), (0, n_r - 1)
        theirs = (n_r + 1, 0)

        def row_piece(side, q):
            cut = cuts[q]
            return remote(buf.at[mine[side], cut], buf.at[theirs[side], cut], row_send.at[side, q],
                          row_recv.at[1 - side, q], vert(side))

        def corner(side):
            return remote(cbuf.at[edge_r[side]], buf.at[theirs[side], halo_c], misc_send.at[side],
                          misc_recv.at[1 - side], diag(side))

        def side_col(src):
            return remote(src, buf.at[pl.ds(1, n_r), halo_c], misc_send.at[2], misc_recv.at[2], lateral)

        my_halo_c = jnp.where(at_left, n_c + 1, 0)
        lands = (0, n_r + 1)

        def row_landing(side, q):
            cut = cuts[q]
            return remote(buf.at[mine[side], cut], buf.at[lands[side], cut], row_send.at[side, q],
                          row_recv.at[side, q], vert(side))

        def corner_landing(side):
            return remote(cbuf.at[edge_r[side]], buf.at[lands[side], my_halo_c], misc_send.at[side],
                          misc_recv.at[side], diag(side))

        def side_landing(src):
            return remote(src, buf.at[pl.ds(1, n_r), my_halo_c], misc_send.at[2], misc_recv.at[2], lateral)

        return row_piece, corner, side_col, row_landing, corner_landing, side_landing

    def by_side(side_pred, fn):
        for side in (0, 1):
            pl.when(jnp.logical_and(side_pred(side), has[side]))(functools.partial(fn, side))

    is_slow = lambda side: odd == side
    is_fast = lambda side: odd != side

    def send_corner(h, pred):
        by_side(pred, lambda side: h[1](side).start())

    def produce_row(h, pred, make, tail=None):
        make(0)
        for q in range(1, NQ):
            make(q)
            by_side(pred, lambda side, q=q: h[0](side, q - 1).start())
        if tail is not None:
            tail()
        by_side(pred, lambda side: h[0](side, NQ - 1).start())

    def wait_row(h, pred, first, pieces):
        def go(side):
            if first:
                h[4](side).wait_recv()
            for q in pieces:
                h[3](side, q).wait_recv()
        by_side(pred, go)

    def drain_row(h, pred):
        def go(side):
            for q in range(NQ):
                h[0](side, q).wait_send()
            h[1](side).wait_send()
        by_side(pred, go)

    def all_sum(layer, s1, s2, fold):
        s1 = jnp.sum(s1, axis=0, keepdims=True)
        s2 = jnp.sum(s2, axis=0, keepdims=True)
        both = jnp.concatenate([s1, s2], axis=0)
        if fold:
            half = both[:, :ca] + both[:, ca:]
            both = jnp.concatenate([half, half], axis=1)
        stat[layer, me] = both
        sends = [remote(stat.at[layer, me], stat.at[layer, me], st_send.at[layer, d], st_recv.at[layer, d], peer(d))
                 for d in range(1, n_dev)]
        for s in sends:
            s.start()
        for d in range(1, n_dev):
            src = (me + n_dev - d) % n_dev
            remote(stat.at[layer, src], stat.at[layer, src], st_send.at[layer, d], st_recv.at[layer, d], peer(d)).wait_recv()
        for s in sends:
            s.wait_send()
        total = stat[layer, 0]
        for k in range(1, n_dev):
            total = total + stat[layer, k]
        return total

    def affine(total, num, gamma, beta):
        mean = total[0:1] / num
        var = total[1:2] / num - mean * mean
        scale = gamma * lax.rsqrt(var + EPS)
        return scale, beta - mean * scale, jnp.zeros_like(beta)

    def group(n, q):
        return (0, n) if q is None else (((0,) + FRAC)[q] * n // 8, FRAC[q] * n // 8)

    def load_x_row(r):
        x_copy(r).wait()

        def blk(c, carry):
            c0 = pl.multiple_of(c * 16, 16)
            for i in range(imgs):
                stg[0, pl.ds(i * 17, 16), :] = xv[i, r, pl.ds(c0, 16), :].astype(F32)
            for k in range(16):
                z[r, pl.ds(pl.multiple_of(c * (8 * imgs), 8 * imgs) + (k // 2) * imgs, imgs),
                  (k % 2) * ca:(k % 2 + 1) * ca] = stg[0, pl.ds(k, imgs, stride=17), :]
            return carry

        lax.fori_loop(0, cols // 16, blk, 0)

    def apply_bn(zz, aff):
        scale, shift, low = aff
        return jnp.maximum(zz * scale + shift, low)

    JN = 8

    def norm_a(r, p, aff):
        off = p * imgs if isinstance(p, int) else pl.multiple_of(p * imgs, JN * imgs)
        y = apply_bn(z[r, pl.ds(off, JN * imgs), :], aff).astype(BF16).reshape(JN, imgs, 2 * ca)
        y = jnp.stack([y[:, :, :ca], y[:, :, ca:]], axis=1).reshape(2 * JN, imgs, ca)
        act[r + 1, pl.ds(1 + 2 * p, 2 * JN)] = y

    def norm_row_a(r, aff, q=None):
        def blk(c, carry):
            norm_a(r, c * JN, aff)
            return carry
        lax.fori_loop(*group(pairs // JN, q), blk, 0)

    def norm_row_b(r, aff, q=None):
        def blk(c, carry):
            zz = z[r, pl.ds(pl.multiple_of(c * (JN * imgs), JN * imgs), JN * imgs), :]
            actb[r + 1, pl.ds(1 + c * JN, JN)] = apply_bn(zz, aff).astype(BF16).reshape(JN, imgs, cb)
            return carry
        lax.fori_loop(*group(cols_b // JN, q), blk, 0)

    def norm_col_a(aff):
        p = jnp.where(at_left, pairs - 1, 0)
        for r in range(rows):
            y = apply_bn(z[r, pl.ds(pl.multiple_of(p * imgs, imgs), imgs), :], aff).astype(BF16)
            cbuf_a[r] = jnp.where(at_left, y[:, ca:], y[:, :ca])

    def norm_col_b(aff):
        p = jnp.where(at_left, cols_b - 1, 0)
        for r in range(rows_b):
            cbuf_b[r] = apply_bn(z[r, pl.ds(pl.multiple_of(p * imgs, imgs), imgs), :], aff).astype(BF16)

    def put(r, c0, n_c, acc, s):
        off = c0 * imgs if isinstance(c0, int) else pl.multiple_of(c0 * imgs, 8 * imgs)
        z[r, pl.ds(off, n_c * imgs), :] = acc
        a3 = acc.reshape(n_c * imgs // 8, 8, acc.shape[-1])
        return s[0] + jnp.sum(a3, axis=0), s[1] + jnp.sum(a3 * a3, axis=0)

    JC = 16
    NC_A, NC_B = pairs // JC, cols_b // JC

    def conv_a(layer, r, c0, s, n=JC):
        parts = []
        for dy in range(3):
            v = act[r + dy, 2 * c0:2 * c0 + 2 * n + 2].reshape(n + 1, 2, imgs, ca)
            for c in range(4):
                parts.append(v[c // 2:c // 2 + n, c % 2].reshape(n * imgs, ca))
        acc = jnp.dot(jnp.concatenate(parts, axis=1), wp[layer], preferred_element_type=F32)
        return put(r, c0, n, acc, s)

    def conv_d(i, c0, s, n=JC):
        first, last = [], []
        for dy in range(3):
            v = act[2 * i + dy + 1, 2 * c0 + 1:2 * c0 + 2 * n + 2]
            a = v[:2 * n].reshape(n, 2, imgs, ca)
            b = v[1:].reshape(n, 2, imgs, ca)
            first += [a[:, 0].reshape(n * imgs, ca), a[:, 1].reshape(n * imgs, ca)]
            last.append(b[:, 1].reshape(n * imgs, ca))
        acc = jnp.dot(jnp.concatenate(first + last, axis=1), wdp[...], preferred_element_type=F32)
        return put(i, c0, n, acc, s)

    def conv_b(layer, r, c0, s, n=JC):
        parts = []
        for dy in range(3):
            for dx in range(3):
                parts.append(actb[r + dy, c0 + dx:c0 + dx + n].reshape(n * imgs, cb))
        acc = jnp.dot(jnp.concatenate(parts, axis=1), wbv[layer], preferred_element_type=F32)
        return put(r, c0, n, acc, s)

    def slow_parts(n_c):
        for q in range(NQ):
            lo, hi = group(n_c, q)
            yield q, [(lo, (hi - lo) // 2), ((lo + hi) // 2, (hi - lo) // 2)]

    zero_stat = lambda: (jnp.zeros((8, 256), F32), jnp.zeros((8, 256), F32))

    for c in early:
        c.wait()

    for layer in range(la):
        for dy in range(3):
            for c in range(4):
                k0 = (dy * 4 + c) * ca
                zero = jnp.zeros((ca, ca), BF16)
                wp[layer, k0:k0 + ca, :ca] = wa_ref[layer, dy, c] if c < 3 else zero
                wp[layer, k0:k0 + ca, ca:] = wa_ref[layer, dy, c - 1] if c > 0 else zero

    num_a = float(imgs * rows * cols * n_dev)
    num_b = float(imgs * rows_b * cols_b * n_dev)

    def dup(v):
        return jnp.concatenate([v, v], axis=1)

    ha = halo(act, cbuf_a, rows, cols)
    halves = ((0, range(0, 2)), (1, range(2, NQ)))

    def layer_a(layer, aff):
        norm_col_a(aff)
        norm_row_a(slow_row, aff, 0)
        send_corner(ha, is_slow)
        ha[2](cbuf_a).start()
        send_corner(ha, is_fast)
        produce_row(ha, is_slow, lambda q: norm_row_a(slow_row, aff, q) if q else None)
        produce_row(ha, is_fast, lambda q: norm_row_a(fast_row, aff, q))

        s = zero_stat()
        mid = [j * JC for j in range(NC_A // 4, NC_A - NC_A // 4)]
        outer = [j * JC for j in range(NC_A) if j * JC not in mid]
        inner = range(1, rows - 1)
        first = range(mid[0] - JN, mid[-1] + JC + 1, JN)
        rest = [(r, p) for r in inner for p in range(0, pairs, JN) if p not in first]
        ready = {r: [(r, p) for p in first] for r in inner}
        for pos, r in enumerate(inner):
            if pos == 0:
                start = sorted(ready[r] + ready[r + 1], key=lambda rp: rp[1])
                now = [start[:8], start[8:]]
                for rp in now[0]:
                    norm_a(*rp, aff)
            for u, c0 in enumerate(mid):
                if pos == 0 and u == 1:
                    for rp in now[1]:
                        norm_a(*rp, aff)
                s = conv_a(layer, r, c0, s)
                todo = ready.get(r + 2)
                if todo is None:
                    todo, left = rest, len(inner) - pos
                    take = -(-len(todo) // ((left - 1) * len(mid) + len(mid) - u))
                else:
                    take = -(-len(todo) // (len(mid) - u))
                for rp in todo[:take]:
                    norm_a(*rp, aff)
                del todo[:take]

        ha[5](cbuf_a).wait_recv()
        wait_row(ha, is_fast, True, range(NQ))
        for r in inner:
            for c0 in outer:
                s = conv_a(layer, r, c0, s)
        for j in range(NC_A):
            s = conv_a(layer, fast_row, j * JC, s)
        for part, pieces in halves:
            wait_row(ha, is_slow, part == 0, pieces)
            for j in range(part * NC_A // 2, (part + 1) * NC_A // 2):
                s = conv_a(layer, slow_row, j * JC, s)
        total = all_sum(layer, *s, True)
        drain_row(ha, is_slow)
        drain_row(ha, is_fast)
        ha[2](cbuf_a).wait_send()
        return affine(total, num_a, dup(bna_ref[layer, 0:1]), dup(bna_ref[layer, 1:2]))

    load_x_row(slow_row)
    load_x_row(fast_row)
    lax.fori_loop(1, rows - 1, lambda r, c: (load_x_row(r), c)[1], 0)
    flat = jnp.zeros((1, 2 * ca), F32)
    aff = lax.fori_loop(0, la, layer_a, (flat + 1.0, flat, flat - jnp.inf))

    norm_col_a(aff)
    norm_row_a(0, aff, 0)

    @pl.when(sp2 == 1)
    def _():
        pl.when(has_up)(lambda: ha[1](0).start())
        ha[2](cbuf_a).start()

    for q in range(1, NQ):
        norm_row_a(0, aff, q)
        pl.when(has_up)(lambda q=q: ha[0](0, q - 1).start())
    pl.when(has_up)(lambda: ha[0](0, NQ - 1).start())

    def inner_d(r, c):
        norm_row_a(r, aff)
        return c

    lax.fori_loop(1, rows, inner_d, 0)
    for c in w_copies:
        c.wait()

    s = zero_stat()
    for i in range(rows_b - 1):
        for c0 in range(0, cols_b - JC, JC):
            s = conv_d(i, c0, s)
    pl.when(sp2 == 0)(lambda: ha[5](cbuf_a).wait_recv())
    for i in range(rows_b - 1):
        for c0 in (cols_b - JC, cols_b - JC // 2):
            s = conv_d(i, c0, s, JC // 2)
    for q, chunks in slow_parts(cols_b):
        @pl.when(has_down)
        def _():
            if q == 0:
                pl.when(sp2 == 0)(lambda: ha[4](1).wait_recv())
            ha[3](1, q).wait_recv()
        for c0, n in chunks:
            s = conv_d(rows_b - 1, c0, s, n)
    total = all_sum(la, *s, False)

    @pl.when(has_up)
    def _():
        for q in range(NQ):
            ha[0](0, q).wait_send()
        pl.when(sp2 == 1)(lambda: ha[1](0).wait_send())

    @pl.when(sp2 == 1)
    def _():
        ha[2](cbuf_a).wait_send()

    aff = affine(total, num_b, bnd_ref[0:1], bnd_ref[1:2])

    hb = halo(actb, cbuf_b, rows_b, cols_b)
    slow_b = odd * (rows_b - 1)
    fast_b = (rows_b - 1) - slow_b

    def layer_b(layer, aff):
        norm_col_b(aff)
        norm_row_b(slow_b, aff, 0)
        send_corner(hb, is_slow)
        hb[2](cbuf_b).start()
        send_corner(hb, is_fast)
        produce_row(hb, is_slow, lambda q: norm_row_b(slow_b, aff, q) if q else None)
        produce_row(hb, is_fast, lambda q: norm_row_b(fast_b, aff, q))

        def inner(r, c):
            norm_row_b(r, aff)
            return c
        lax.fori_loop(1, rows_b - 1, inner, 0)
        s = zero_stat()
        for r in range(1, rows_b - 1):
            for c0 in range(JC, cols_b - JC, JC):
                s = conv_b(layer, r, c0, s)
        hb[5](cbuf_b).wait_recv()
        wait_row(hb, is_fast, True, range(NQ))
        for r in range(1, rows_b - 1):
            for c0 in (0, cols_b - JC):
                s = conv_b(layer, r, c0, s)
        for c0 in range(0, cols_b, JC):
            s = conv_b(layer, fast_b, c0, s)
        for q, chunks in slow_parts(cols_b):
            wait_row(hb, is_slow, q == 0, [q])
            for c0, n in chunks:
                s = conv_b(layer, slow_b, c0, s, n)
        total = all_sum(la + 1 + layer, *s, False)
        drain_row(hb, is_slow)
        drain_row(hb, is_fast)
        hb[2](cbuf_b).wait_send()
        return affine(total, num_b, bnb_ref[layer, 0:1], bnb_ref[layer, 1:2])

    aff = lax.fori_loop(0, lb, layer_b, aff)

    def final_row(r, carry):
        def blk(c, carry):
            c0 = pl.multiple_of(c * 16, 16)
            for k in range(16):
                y = apply_bn(z[r, pl.ds(pl.multiple_of(c0 * imgs + k * imgs, imgs), imgs), :], aff)
                for h in range(2):
                    stg[h, pl.ds(k * 33, imgs), :] = y[:, h * 128:(h + 1) * 128]
            for i in range(imgs):
                for h in range(2):
                    y_ref[i, r, pl.ds(c0, 16), h * 128:(h + 1) * 128] = stg[h, pl.ds(i, 16, stride=33), :].astype(BF16)
            return carry
        return lax.fori_loop(0, cols_b // 16, blk, carry)

    lax.fori_loop(0, rows_b, final_row, 0)


def solution(mesh):
    rows_n, cols_n = mesh.shape["sp"], mesh.shape["sp2"]

    def per_device(x, w_a, bn_a, w_down, bn_down, w_b, bn_b):
        imgs, rows, cols, ca = x.shape
        cb = w_down.shape[-1]
        la, lb = w_a.shape[0], w_b.shape[0]
        rows_b, cols_b = rows // 2, cols // 2
        dims = (imgs, rows, cols, ca, cb, la, lb, rows_n, cols_n)
        n_dev = rows_n * cols_n
        layers = la + 1 + lb
        vm = pl.BlockSpec(memory_space=pltpu.VMEM)
        hbm = pl.BlockSpec(memory_space=pl.ANY)
        dma = pltpu.SemaphoreType.DMA
        return pl.pallas_call(
            functools.partial(stack_kernel, dims),
            out_shape=pltpu.VMEM((imgs, rows_b, cols_b, cb), BF16),
            in_specs=[hbm] * 7,
            out_specs=vm,
            scratch_shapes=[
                pltpu.VMEM(w_a.shape, BF16),
                pltpu.VMEM(bn_a.shape, F32), pltpu.VMEM(bn_down.shape, F32), pltpu.VMEM(bn_b.shape, F32),
                pltpu.VMEM((imgs, rows, cols, ca), BF16),
                pltpu.VMEM((rows + 2, cols + 2, imgs, ca), BF16),
                pltpu.VMEM((rows_b + 2, cols_b + 2, imgs, cb), BF16),
                pltpu.VMEM((rows, cols // 2 * imgs, 2 * ca), F32),
                pltpu.VMEM((2, imgs * 17 + 16, 128), F32),
                pltpu.VMEM((la, 12 * ca, 2 * ca), BF16),
                pltpu.VMEM((9 * ca, cb), BF16),
                pltpu.VMEM((lb, 9 * cb, cb), BF16),
                pltpu.VMEM((rows, imgs, ca), BF16),
                pltpu.VMEM((rows_b, imgs, cb), BF16),
                pltpu.VMEM((layers, n_dev, 2, 256), F32),
                dma((rows,)), dma((14,)),
                dma((2, NQ)), dma((2, NQ)), dma((3,)), dma((3,)), dma((layers, n_dev)), dma((layers, n_dev)),
            ],
            compiler_params=pltpu.CompilerParams(
                collective_id=0, has_side_effects=True, vmem_limit_bytes=58_000_000),
            name="stack",
        )(x, w_a, bn_a, w_down, bn_down, w_b.reshape(lb, 9 * cb, cb), bn_b)

    tile_spec = P("dp", "sp", "sp2", None)
    return jax.shard_map(per_device, mesh=mesh, in_specs=(tile_spec, P(), P(), P(), P(), P(), P()),
                         out_specs=tile_spec, check_vma=False)
```

```python
import functools

import jax
import jax.numpy as jnp
from jax import lax
from jax.experimental import pallas as pl
from jax.experimental.pallas import tpu as pltpu
from jax.sharding import PartitionSpec as P

EPS = 1e-5
FRAC = (1, 3, 5, 7, 8)
NQ = len(FRAC)
F32 = jnp.float32
BF16 = jnp.bfloat16


def stack_kernel(dims, x_hbm, wa_hbm, bna_hbm, wd_ref, bnd_hbm, wb_ref, bnb_hbm, y_ref,
                 wa_ref, bna_ref, bnd_ref, bnb_ref, xv, act, actb, z, stg, wp, wdp, wbv, cbuf_a, cbuf_b, stat,
                 zhalo, x_sem, w_sem, z_send, z_recv, row_send, row_recv, misc_send, misc_recv, st_send, st_recv):
    imgs, rows, cols, ca, cb, la, lb, rows_n, cols_n = dims
    n_dev = rows_n * cols_n
    pairs = cols // 2
    rows_b, cols_b = rows // 2, cols // 2
    sp, sp2 = lax.axis_index("sp"), lax.axis_index("sp2")
    me = sp2 * rows_n + sp
    odd = sp % 2
    has_up, has_down = sp > 0, sp < rows_n - 1
    has = {0: has_up, 1: has_down}
    at_left = sp2 == 0

    def x_copy(r):
        return pltpu.make_async_copy(x_hbm.at[:, r], xv.at[:, r], x_sem.at[r])

    slow_row = odd * (rows - 1)
    fast_row = (rows - 1) - slow_row
    x_copy(slow_row).start()
    x_copy(fast_row).start()
    for r in range(1, rows - 1):
        x_copy(r).start()

    early = [pltpu.make_async_copy(a, b, w_sem.at[10 + k]) for k, (a, b) in enumerate(
        ((wa_hbm, wa_ref), (bna_hbm, bna_ref), (bnd_hbm, bnd_ref), (bnb_hbm, bnb_ref)))]
    for c in early:
        c.start()

    order = [(dy, dx) for dy in range(3) for dx in range(2)] + [(dy, 2) for dy in range(3)]
    w_copies = [pltpu.make_async_copy(wd_ref.at[dy, dx], wdp.at[pl.ds(k * ca, ca)], w_sem.at[k])
                for k, (dy, dx) in enumerate(order)]
    w_copies.append(pltpu.make_async_copy(wb_ref, wbv, w_sem.at[9]))
    for c in w_copies:
        c.start()

    act[0] = jnp.zeros((cols + 2, imgs, ca), BF16)
    act[rows + 1] = jnp.zeros((cols + 2, imgs, ca), BF16)
    actb[0] = jnp.zeros((cols_b + 2, imgs, cb), BF16)
    actb[rows_b + 1] = jnp.zeros((cols_b + 2, imgs, cb), BF16)
    for r in range(1, rows + 1):
        for c in (0, cols + 1):
            act[r, c] = jnp.zeros((imgs, ca), BF16)
    for r in range(1, rows_b + 1):
        for c in (0, cols_b + 1):
            actb[r, c] = jnp.zeros((imgs, cb), BF16)

    barrier = pltpu.get_barrier_semaphore()

    def peer(d):
        q = (me + d) % n_dev
        return {"sp2": q // rows_n, "sp": q % rows_n}

    for d in range(1, n_dev):
        pl.semaphore_signal(barrier, inc=1, device_id=peer(d), device_id_type=pl.DeviceIdType.MESH)
    pl.semaphore_wait(barrier, n_dev - 1)

    def remote(src, dst, ssem, rsem, dev):
        return pltpu.make_async_remote_copy(src_ref=src, dst_ref=dst, send_sem=ssem, recv_sem=rsem,
                                            device_id=dev, device_id_type=pl.DeviceIdType.MESH)

    def vert(side):
        return {"sp": sp - 1 if side == 0 else sp + 1, "sp2": sp2}

    def diag(side):
        return {"sp": sp - 1 if side == 0 else sp + 1, "sp2": 1 - sp2}

    lateral = {"sp": sp, "sp2": 1 - sp2}

    def halo(buf, cbuf, n_r, n_c):
        ends = [f * n_c // 8 + 2 for f in FRAC[:-1]] + [n_c + 1]
        cuts = [pl.ds(a, b - a) for a, b in zip([1] + ends[:-1], ends)]
        halo_c = jnp.where(at_left, 0, n_c + 1)
        mine, edge_r = (1, n_r), (0, n_r - 1)
        theirs = (n_r + 1, 0)

        def row_piece(side, q):
            cut = cuts[q]
            return remote(buf.at[mine[side], cut], buf.at[theirs[side], cut], row_send.at[side, q],
                          row_recv.at[1 - side, q], vert(side))

        def corner(side):
            return remote(cbuf.at[edge_r[side]], buf.at[theirs[side], halo_c], misc_send.at[side],
                          misc_recv.at[1 - side], diag(side))

        def side_col(src):
            return remote(src, buf.at[pl.ds(1, n_r), halo_c], misc_send.at[2], misc_recv.at[2], lateral)

        my_halo_c = jnp.where(at_left, n_c + 1, 0)
        lands = (0, n_r + 1)

        def row_landing(side, q):
            cut = cuts[q]
            return remote(buf.at[mine[side], cut], buf.at[lands[side], cut], row_send.at[side, q],
                          row_recv.at[side, q], vert(side))

        def corner_landing(side):
            return remote(cbuf.at[edge_r[side]], buf.at[lands[side], my_halo_c], misc_send.at[side],
                          misc_recv.at[side], diag(side))

        def side_landing(src):
            return remote(src, buf.at[pl.ds(1, n_r), my_halo_c], misc_send.at[2], misc_recv.at[2], lateral)

        return row_piece, corner, side_col, row_landing, corner_landing, side_landing

    def by_side(side_pred, fn):
        for side in (0, 1):
            pl.when(jnp.logical_and(side_pred(side), has[side]))(functools.partial(fn, side))

    is_slow = lambda side: odd == side
    is_fast = lambda side: odd != side

    def send_corner(h, pred):
        by_side(pred, lambda side: h[1](side).start())

    def produce_row(h, pred, make, skip=0):
        make(0)
        for q in range(1, NQ):
            make(q)
            if q > skip:
                by_side(pred, lambda side, q=q: h[0](side, q - 1).start())
        by_side(pred, lambda side: h[0](side, NQ - 1).start())

    def wait_row(h, pred, first, pieces):
        def go(side):
            if first:
                h[4](side).wait_recv()
            for q in pieces:
                h[3](side, q).wait_recv()
        by_side(pred, go)

    def drain_row(h, pred, skip=0):
        def go(side):
            for q in range(skip, NQ):
                h[0](side, q).wait_send()
            h[1](side).wait_send()
        by_side(pred, go)

    zn = (cols_b // 8 + 1) * imgs
    slow_dev = sp + 2 * odd - 1
    has_slow = jnp.logical_and(slow_dev >= 0, slow_dev < rows_n)
    slow_up = jnp.logical_and(has_slow, odd == 0)
    slow_down = jnp.logical_and(has_slow, odd == 1)

    def z_copy(t, row):
        return remote(z.at[row, pl.ds(0, zn)], zhalo.at[t], z_send.at[t], z_recv.at[t],
                      {"sp": slow_dev, "sp2": sp2})

    def all_sum(layer, s1, s2, fold, ahead=lambda: None):
        s1 = jnp.sum(s1, axis=0, keepdims=True)
        s2 = jnp.sum(s2, axis=0, keepdims=True)
        both = jnp.concatenate([s1, s2], axis=0)
        if fold:
            half = both[:, :ca] + both[:, ca:]
            both = jnp.concatenate([half, half], axis=1)
        stat[layer, me] = both
        sends = [remote(stat.at[layer, me], stat.at[layer, me], st_send.at[layer, d], st_recv.at[layer, d], peer(d))
                 for d in range(1, n_dev)]
        for s in sends:
            s.start()
        ahead()
        for d in range(1, n_dev):
            src = (me + n_dev - d) % n_dev
            remote(stat.at[layer, src], stat.at[layer, src], st_send.at[layer, d], st_recv.at[layer, d], peer(d)).wait_recv()
        for s in sends:
            s.wait_send()
        total = stat[layer, 0]
        for k in range(1, n_dev):
            total = total + stat[layer, k]
        return total

    def affine(total, num, gamma, beta):
        mean = total[0:1] / num
        var = total[1:2] / num - mean * mean
        scale = gamma * lax.rsqrt(var + EPS)
        return scale, beta - mean * scale, jnp.zeros_like(beta)

    def group(n, q):
        return (0, n) if q is None else (((0,) + FRAC)[q] * n // 8, FRAC[q] * n // 8)

    def load_x_row(r):
        x_copy(r).wait()

        def blk(c, carry):
            c0 = pl.multiple_of(c * 16, 16)
            for i in range(imgs):
                stg[0, pl.ds(i * 17, 16), :] = xv[i, r, pl.ds(c0, 16), :].astype(F32)
            for k in range(16):
                z[r, pl.ds(pl.multiple_of(c * (8 * imgs), 8 * imgs) + (k // 2) * imgs, imgs),
                  (k % 2) * ca:(k % 2 + 1) * ca] = stg[0, pl.ds(k, imgs, stride=17), :]
            return carry

        lax.fori_loop(0, cols // 16, blk, 0)

    def apply_bn(zz, aff):
        scale, shift, low = aff
        return jnp.maximum(zz * scale + shift, low)

    JN = 8

    def norm_a(r, p, aff):
        off = p * imgs if isinstance(p, int) else pl.multiple_of(p * imgs, JN * imgs)
        y = apply_bn(z[r, pl.ds(off, JN * imgs), :], aff).astype(BF16).reshape(JN, imgs, 2 * ca)
        y = jnp.stack([y[:, :, :ca], y[:, :, ca:]], axis=1).reshape(2 * JN, imgs, ca)
        act[r + 1, pl.ds(1 + 2 * p, 2 * JN)] = y

    def norm_row_a(r, aff, q=None):
        def blk(c, carry):
            norm_a(r, c * JN, aff)
            return carry
        lax.fori_loop(*group(pairs // JN, q), blk, 0)

    def norm_row_b(r, aff, q=None):
        def blk(c, carry):
            zz = z[r, pl.ds(pl.multiple_of(c * (JN * imgs), JN * imgs), JN * imgs), :]
            actb[r + 1, pl.ds(1 + c * JN, JN)] = apply_bn(zz, aff).astype(BF16).reshape(JN, imgs, cb)
            return carry
        lax.fori_loop(*group(cols_b // JN, q), blk, 0)

    def norm_col_a(aff):
        p = jnp.where(at_left, pairs - 1, 0)
        for r in range(rows):
            y = apply_bn(z[r, pl.ds(pl.multiple_of(p * imgs, imgs), imgs), :], aff).astype(BF16)
            cbuf_a[r] = jnp.where(at_left, y[:, ca:], y[:, :ca])

    def norm_col_b(aff):
        p = jnp.where(at_left, cols_b - 1, 0)
        for r in range(rows_b):
            cbuf_b[r] = apply_bn(z[r, pl.ds(pl.multiple_of(p * imgs, imgs), imgs), :], aff).astype(BF16)

    def put(r, c0, n_c, acc, s):
        off = c0 * imgs if isinstance(c0, int) else pl.multiple_of(c0 * imgs, 8 * imgs)
        z[r, pl.ds(off, n_c * imgs), :] = acc
        a3 = acc.reshape(n_c * imgs // 8, 8, acc.shape[-1])
        return s[0] + jnp.sum(a3, axis=0), s[1] + jnp.sum(a3 * a3, axis=0)

    JC = 16
    NC_A, NC_B = pairs // JC, cols_b // JC

    def conv_a(layer, r, c0, s, n=JC):
        parts = []
        for dy in range(3):
            v = act[r + dy, 2 * c0:2 * c0 + 2 * n + 2].reshape(n + 1, 2, imgs, ca)
            for c in range(4):
                parts.append(v[c // 2:c // 2 + n, c % 2].reshape(n * imgs, ca))
        acc = jnp.dot(jnp.concatenate(parts, axis=1), wp[layer], preferred_element_type=F32)
        return put(r, c0, n, acc, s)

    def conv_d(i, c0, s, n=JC):
        first, last = [], []
        for dy in range(3):
            v = act[2 * i + dy + 1, 2 * c0 + 1:2 * c0 + 2 * n + 2]
            a = v[:2 * n].reshape(n, 2, imgs, ca)
            b = v[1:].reshape(n, 2, imgs, ca)
            first += [a[:, 0].reshape(n * imgs, ca), a[:, 1].reshape(n * imgs, ca)]
            last.append(b[:, 1].reshape(n * imgs, ca))
        acc = jnp.dot(jnp.concatenate(first + last, axis=1), wdp[...], preferred_element_type=F32)
        return put(i, c0, n, acc, s)

    def conv_b(layer, r, c0, s, n=JC):
        parts = []
        for dy in range(3):
            for dx in range(3):
                parts.append(actb[r + dy, c0 + dx:c0 + dx + n].reshape(n * imgs, cb))
        acc = jnp.dot(jnp.concatenate(parts, axis=1), wbv[layer], preferred_element_type=F32)
        return put(r, c0, n, acc, s)

    def slow_parts(n_c):
        for q in range(NQ):
            lo, hi = group(n_c, q)
            yield q, [(lo, (hi - lo) // 2), ((lo + hi) // 2, (hi - lo) // 2)]

    zero_stat = lambda: (jnp.zeros((8, 256), F32), jnp.zeros((8, 256), F32))

    for c in early:
        c.wait()

    for layer in range(la):
        for dy in range(3):
            for c in range(4):
                k0 = (dy * 4 + c) * ca
                zero = jnp.zeros((ca, ca), BF16)
                wp[layer, k0:k0 + ca, :ca] = wa_ref[layer, dy, c] if c < 3 else zero
                wp[layer, k0:k0 + ca, ca:] = wa_ref[layer, dy, c - 1] if c > 0 else zero

    num_a = float(imgs * rows * cols * n_dev)
    num_b = float(imgs * rows_b * cols_b * n_dev)

    def dup(v):
        return jnp.concatenate([v, v], axis=1)

    ha = halo(act, cbuf_a, rows, cols)
    halves = ((0, range(0, 3)), (1, range(3, NQ)))

    def layer_a(layer, aff):
        norm_col_a(aff)
        norm_row_a(slow_row, aff, 0)
        send_corner(ha, is_slow)
        ha[2](cbuf_a).start()
        send_corner(ha, is_fast)
        produce_row(ha, is_slow, lambda q: norm_row_a(slow_row, aff, q) if q else None)
        produce_row(ha, is_fast, lambda q: norm_row_a(fast_row, aff, q))

        s = zero_stat()
        mid = [j * JC for j in range(NC_A // 4, NC_A - NC_A // 4)]
        outer = [j * JC for j in range(NC_A) if j * JC not in mid]
        inner = range(1, rows - 1)
        first = range(mid[0] - JN, mid[-1] + JC + 1, JN)
        rest = [(r, p) for r in inner for p in range(0, pairs, JN) if p not in first]
        ready = {r: [(r, p) for p in first] for r in inner}
        for pos, r in enumerate(inner):
            if pos == 0:
                start = sorted(ready[r] + ready[r + 1], key=lambda rp: rp[1])
                now = [start[:8], start[8:]]
                for rp in now[0]:
                    norm_a(*rp, aff)
            for u, c0 in enumerate(mid):
                if pos == 0 and u == 1:
                    for rp in now[1]:
                        norm_a(*rp, aff)
                s = conv_a(layer, r, c0, s)
                todo = ready.get(r + 2)
                if todo is None:
                    todo, left = rest, len(inner) - pos
                    take = -(-len(todo) // ((left - 1) * len(mid) + len(mid) - u))
                else:
                    take = -(-len(todo) // (len(mid) - u))
                for rp in todo[:take]:
                    norm_a(*rp, aff)
                del todo[:take]

        ha[5](cbuf_a).wait_recv()
        wait_row(ha, is_fast, True, range(NQ))
        for r in inner:
            for c0 in outer:
                s = conv_a(layer, r, c0, s)
        for j in range(NC_A):
            s = conv_a(layer, fast_row, j * JC, s)
        for part, pieces in halves:
            wait_row(ha, is_slow, part == 0, pieces)
            for j in range(part * NC_A // 2, (part + 1) * NC_A // 2):
                s = conv_a(layer, slow_row, j * JC, s)
        total = all_sum(layer, *s, True, lambda: pl.when(jnp.logical_and(slow_up, layer == la - 1))(
            lambda: z_copy(0, 0).start()))
        drain_row(ha, is_slow)
        drain_row(ha, is_fast)
        ha[2](cbuf_a).wait_send()
        return affine(total, num_a, dup(bna_ref[layer, 0:1]), dup(bna_ref[layer, 1:2]))

    load_x_row(slow_row)
    load_x_row(fast_row)
    lax.fori_loop(1, rows - 1, lambda r, c: (load_x_row(r), c)[1], 0)
    flat = jnp.zeros((1, 2 * ca), F32)
    aff = lax.fori_loop(0, la, layer_a, (flat + 1.0, flat, flat - jnp.inf))

    norm_col_a(aff)
    norm_row_a(0, aff, 0)

    @pl.when(sp2 == 1)
    def _():
        pl.when(has_up)(lambda: ha[1](0).start())
        ha[2](cbuf_a).start()

    fast_up = jnp.logical_and(has_up, odd == 1)
    fast_down = jnp.logical_and(has_down, odd == 0)
    for q in range(1, NQ):
        norm_row_a(0, aff, q)
        pl.when(has_up if q > 1 else fast_up)(lambda q=q: ha[0](0, q - 1).start())
    pl.when(has_up)(lambda: ha[0](0, NQ - 1).start())

    def inner_d(r, c):
        norm_row_a(r, aff)
        return c

    lax.fori_loop(1, rows, inner_d, 0)
    for c in w_copies:
        c.wait()

    pl.when(slow_up)(lambda: z_copy(0, 0).wait_send())
    s = zero_stat()
    for i in range(rows_b - 1):
        for c0 in range(0, cols_b - JC, JC):
            s = conv_d(i, c0, s)

    @pl.when(slow_down)
    def _():
        z_copy(0, 0).wait_recv()
        y = apply_bn(zhalo[0], aff).astype(BF16).reshape(zn // imgs, imgs, 2 * ca)
        y = jnp.stack([y[:, :, :ca], y[:, :, ca:]], axis=1).reshape(2 * zn // imgs, imgs, ca)
        act[rows + 1, 1:cols // 8 + 2] = y[:cols // 8 + 1]

    pl.when(sp2 == 0)(lambda: ha[5](cbuf_a).wait_recv())
    for i in range(rows_b - 1):
        for c0 in (cols_b - JC, cols_b - JC // 2):
            s = conv_d(i, c0, s, JC // 2)
    for q, chunks in slow_parts(cols_b):
        if q == 0:
            pl.when(jnp.logical_and(has_down, sp2 == 0))(lambda: ha[4](1).wait_recv())
        pl.when(has_down if q else fast_down)(lambda: ha[3](1, q).wait_recv())
        for c0, n in chunks:
            s = conv_d(rows_b - 1, c0, s, n)
    slow_b = odd * (rows_b - 1)
    total = all_sum(la, *s, False, lambda: pl.when(has_slow)(lambda: z_copy(1, slow_b).start()))

    pl.when(fast_up)(lambda: ha[0](0, 0).wait_send())

    @pl.when(has_up)
    def _():
        for q in range(1, NQ):
            ha[0](0, q).wait_send()
        pl.when(sp2 == 1)(lambda: ha[1](0).wait_send())

    @pl.when(sp2 == 1)
    def _():
        ha[2](cbuf_a).wait_send()

    aff = affine(total, num_b, bnd_ref[0:1], bnd_ref[1:2])

    hb = halo(actb, cbuf_b, rows_b, cols_b)
    fast_b = (rows_b - 1) - slow_b

    def layer_b(layer, aff):
        norm_col_b(aff)
        norm_row_b(slow_b, aff, 0)
        send_corner(hb, is_slow)
        hb[2](cbuf_b).start()
        send_corner(hb, is_fast)
        produce_row(hb, is_slow, lambda q: norm_row_b(slow_b, aff, q) if q else None, 1)
        produce_row(hb, is_fast, lambda q: norm_row_b(fast_b, aff, q))

        def inner(r, c):
            norm_row_b(r, aff)
            return c
        lax.fori_loop(1, rows_b - 1, inner, 0)
        s = zero_stat()
        for r in range(1, rows_b - 1):
            for c0 in range(JC, cols_b - JC, JC):
                s = conv_b(layer, r, c0, s)

        def first_piece(side):
            z_copy(1 + layer, slow_b).wait_send()
            z_copy(1 + layer, slow_b).wait_recv()
            y = apply_bn(zhalo[1 + layer], aff).astype(BF16).reshape(zn // imgs, imgs, cb)
            actb[(0, rows_b + 1)[side], 1:zn // imgs + 1] = y
        by_side(is_slow, first_piece)
        hb[5](cbuf_b).wait_recv()
        wait_row(hb, is_fast, True, range(NQ))
        for r in range(1, rows_b - 1):
            for c0 in (0, cols_b - JC):
                s = conv_b(layer, r, c0, s)
        for c0 in range(0, cols_b, JC):
            s = conv_b(layer, fast_b, c0, s)
        for q, chunks in slow_parts(cols_b):
            wait_row(hb, is_slow, q == 0, [q] if q else [])
            for c0, n in chunks:
                s = conv_b(layer, slow_b, c0, s, n)
        total = all_sum(la + 1 + layer, *s, False, lambda: pl.when(jnp.logical_and(has_slow, layer + 1 < lb))(
            lambda: z_copy(2 + layer, slow_b).start()))
        drain_row(hb, is_slow, 1)
        drain_row(hb, is_fast)
        hb[2](cbuf_b).wait_send()
        return affine(total, num_b, bnb_ref[layer, 0:1], bnb_ref[layer, 1:2])

    aff = lax.fori_loop(0, lb, layer_b, aff)

    def final_row(r, carry):
        def half_block(c0, g):
            for k in range(16):
                y = apply_bn(z[r, pl.ds(pl.multiple_of(c0 * imgs + k * imgs, imgs), imgs), :], aff)
                for h in range(2):
                    stg[g + h, pl.ds(k * 33, imgs), :] = y[:, h * 128:(h + 1) * 128]

        def turn(c0, g):
            for i in range(imgs):
                for h in range(2):
                    y_ref[i, r, pl.ds(c0, 16), h * 128:(h + 1) * 128] = stg[g + h, pl.ds(i, 16, stride=33), :].astype(BF16)

        def blk(c, carry):
            c0 = pl.multiple_of(c * 32, 32)
            half_block(c0, 0)
            half_block(c0 + 16, 2)
            turn(c0, 0)
            turn(pl.multiple_of(c0 + 16, 16), 2)
            return carry
        return lax.fori_loop(0, cols_b // 32, blk, carry)

    lax.fori_loop(0, rows_b, final_row, 0)


def solution(mesh):
    rows_n, cols_n = mesh.shape["sp"], mesh.shape["sp2"]

    def per_device(x, w_a, bn_a, w_down, bn_down, w_b, bn_b):
        imgs, rows, cols, ca = x.shape
        cb = w_down.shape[-1]
        la, lb = w_a.shape[0], w_b.shape[0]
        rows_b, cols_b = rows // 2, cols // 2
        dims = (imgs, rows, cols, ca, cb, la, lb, rows_n, cols_n)
        n_dev = rows_n * cols_n
        layers = la + 1 + lb
        vm = pl.BlockSpec(memory_space=pltpu.VMEM)
        hbm = pl.BlockSpec(memory_space=pl.ANY)
        dma = pltpu.SemaphoreType.DMA
        return pl.pallas_call(
            functools.partial(stack_kernel, dims),
            out_shape=pltpu.VMEM((imgs, rows_b, cols_b, cb), BF16),
            in_specs=[hbm] * 7,
            out_specs=vm,
            scratch_shapes=[
                pltpu.VMEM(w_a.shape, BF16),
                pltpu.VMEM(bn_a.shape, F32), pltpu.VMEM(bn_down.shape, F32), pltpu.VMEM(bn_b.shape, F32),
                pltpu.VMEM((imgs, rows, cols, ca), BF16),
                pltpu.VMEM((rows + 2, cols + 2, imgs, ca), BF16),
                pltpu.VMEM((rows_b + 2, cols_b + 2, imgs, cb), BF16),
                pltpu.VMEM((rows, cols // 2 * imgs, 2 * ca), F32),
                pltpu.VMEM((4, imgs * 17 + 16, 128), F32),
                pltpu.VMEM((la, 12 * ca, 2 * ca), BF16),
                pltpu.VMEM((9 * ca, cb), BF16),
                pltpu.VMEM((lb, 9 * cb, cb), BF16),
                pltpu.VMEM((rows, imgs, ca), BF16),
                pltpu.VMEM((rows_b, imgs, cb), BF16),
                pltpu.VMEM((layers, n_dev, 2, 256), F32),
                pltpu.VMEM((lb + 1, (cols_b // 8 + 1) * imgs, 256), F32),
                dma((rows,)), dma((14,)), dma((lb + 1,)), dma((lb + 1,)),
                dma((2, NQ)), dma((2, NQ)), dma((3,)), dma((3,)), dma((layers, n_dev)), dma((layers, n_dev)),
            ],
            compiler_params=pltpu.CompilerParams(
                collective_id=0, has_side_effects=True, vmem_limit_bytes=58_000_000),
            name="stack",
        )(x, w_a, bn_a, w_down, bn_down, w_b.reshape(lb, 9 * cb, cb), bn_b)

    tile_spec = P("dp", "sp", "sp2", None)
    return jax.shard_map(per_device, mesh=mesh, in_specs=(tile_spec, P(), P(), P(), P(), P(), P()),
                         out_specs=tile_spec, check_vma=False)
```

```python
import functools

import jax
import jax.numpy as jnp
from jax import lax
from jax.experimental import pallas as pl
from jax.experimental.pallas import tpu as pltpu
from jax.sharding import PartitionSpec as P

EPS = 1e-5
FRAC = (1, 3, 5, 7, 8)
NQ = len(FRAC)
F32 = jnp.float32
BF16 = jnp.bfloat16


def stack_kernel(dims, x_hbm, wa_hbm, bna_hbm, wd_ref, bnd_hbm, wb_ref, bnb_hbm, y_ref,
                 wa_ref, bna_ref, bnd_ref, bnb_ref, xv, act, actb, z, stg, wp, wdp, wbv, cbuf_a, cbuf_b, stat,
                 zhalo, x_sem, w_sem, z_send, z_recv, row_send, row_recv, misc_send, misc_recv, st_send, st_recv):
    imgs, rows, cols, ca, cb, la, lb, rows_n, cols_n = dims
    n_dev = rows_n * cols_n
    pairs = cols // 2
    rows_b, cols_b = rows // 2, cols // 2
    sp, sp2 = lax.axis_index("sp"), lax.axis_index("sp2")
    me = sp2 * rows_n + sp
    odd = sp % 2
    has_up, has_down = sp > 0, sp < rows_n - 1
    has = {0: has_up, 1: has_down}
    at_left = sp2 == 0

    def x_copy(r):
        return pltpu.make_async_copy(x_hbm.at[:, r], xv.at[:, r], x_sem.at[r])

    slow_row = odd * (rows - 1)
    fast_row = (rows - 1) - slow_row
    x_copy(slow_row).start()
    x_copy(fast_row).start()
    for r in range(1, rows - 1):
        x_copy(r).start()

    early = [pltpu.make_async_copy(a, b, w_sem.at[10 + k]) for k, (a, b) in enumerate(
        ((wa_hbm, wa_ref), (bna_hbm, bna_ref), (bnd_hbm, bnd_ref), (bnb_hbm, bnb_ref)))]
    for c in early:
        c.start()

    order = [(dy, dx) for dy in range(3) for dx in range(2)] + [(dy, 2) for dy in range(3)]
    w_copies = [pltpu.make_async_copy(wd_ref.at[dy, dx], wdp.at[pl.ds(k * ca, ca)], w_sem.at[k])
                for k, (dy, dx) in enumerate(order)]
    w_copies.append(pltpu.make_async_copy(wb_ref, wbv, w_sem.at[9]))
    for c in w_copies:
        c.start()

    act[0] = jnp.zeros((cols + 2, imgs, ca), BF16)
    act[rows + 1] = jnp.zeros((cols + 2, imgs, ca), BF16)
    actb[0] = jnp.zeros((cols_b + 2, imgs, cb), BF16)
    actb[rows_b + 1] = jnp.zeros((cols_b + 2, imgs, cb), BF16)
    for r in range(1, rows + 1):
        for c in (0, cols + 1):
            act[r, c] = jnp.zeros((imgs, ca), BF16)
    for r in range(1, rows_b + 1):
        for c in (0, cols_b + 1):
            actb[r, c] = jnp.zeros((imgs, cb), BF16)

    barrier = pltpu.get_barrier_semaphore()

    def peer(d):
        q = (me + d) % n_dev
        return {"sp2": q // rows_n, "sp": q % rows_n}

    for d in range(1, n_dev):
        pl.semaphore_signal(barrier, inc=1, device_id=peer(d), device_id_type=pl.DeviceIdType.MESH)
    pl.semaphore_wait(barrier, n_dev - 1)

    def remote(src, dst, ssem, rsem, dev):
        return pltpu.make_async_remote_copy(src_ref=src, dst_ref=dst, send_sem=ssem, recv_sem=rsem,
                                            device_id=dev, device_id_type=pl.DeviceIdType.MESH)

    def vert(side):
        return {"sp": sp - 1 if side == 0 else sp + 1, "sp2": sp2}

    def diag(side):
        return {"sp": sp - 1 if side == 0 else sp + 1, "sp2": 1 - sp2}

    lateral = {"sp": sp, "sp2": 1 - sp2}

    def halo(buf, cbuf, n_r, n_c):
        ends = [f * n_c // 8 + 2 for f in FRAC[:-1]] + [n_c + 1]
        cuts = [pl.ds(a, b - a) for a, b in zip([1] + ends[:-1], ends)]
        halo_c = jnp.where(at_left, 0, n_c + 1)
        mine, edge_r = (1, n_r), (0, n_r - 1)
        theirs = (n_r + 1, 0)

        def row_piece(side, q):
            cut = cuts[q]
            return remote(buf.at[mine[side], cut], buf.at[theirs[side], cut], row_send.at[side, q],
                          row_recv.at[1 - side, q], vert(side))

        def corner(side):
            return remote(cbuf.at[edge_r[side]], buf.at[theirs[side], halo_c], misc_send.at[side],
                          misc_recv.at[1 - side], diag(side))

        def side_col(src):
            return remote(src, buf.at[pl.ds(1, n_r), halo_c], misc_send.at[2], misc_recv.at[2], lateral)

        my_halo_c = jnp.where(at_left, n_c + 1, 0)
        lands = (0, n_r + 1)

        def row_landing(side, q):
            cut = cuts[q]
            return remote(buf.at[mine[side], cut], buf.at[lands[side], cut], row_send.at[side, q],
                          row_recv.at[side, q], vert(side))

        def corner_landing(side):
            return remote(cbuf.at[edge_r[side]], buf.at[lands[side], my_halo_c], misc_send.at[side],
                          misc_recv.at[side], diag(side))

        def side_landing(src):
            return remote(src, buf.at[pl.ds(1, n_r), my_halo_c], misc_send.at[2], misc_recv.at[2], lateral)

        return row_piece, corner, side_col, row_landing, corner_landing, side_landing

    def by_side(side_pred, fn):
        for side in (0, 1):
            pl.when(jnp.logical_and(side_pred(side), has[side]))(functools.partial(fn, side))

    is_slow = lambda side: odd == side
    is_fast = lambda side: odd != side

    def send_corner(h, pred):
        by_side(pred, lambda side: h[1](side).start())

    def produce_row(h, pred, make, skip=0):
        make(0)
        for q in range(1, NQ):
            make(q)
            if q > skip:
                by_side(pred, lambda side, q=q: h[0](side, q - 1).start())
        by_side(pred, lambda side: h[0](side, NQ - 1).start())

    def wait_row(h, pred, first, pieces):
        def go(side):
            if first:
                h[4](side).wait_recv()
            for q in pieces:
                h[3](side, q).wait_recv()
        by_side(pred, go)

    def drain_row(h, pred, skip=0):
        def go(side):
            for q in range(skip, NQ):
                h[0](side, q).wait_send()
            h[1](side).wait_send()
        by_side(pred, go)

    zn = (cols_b // 8 + 1) * imgs
    slow_dev = sp + 2 * odd - 1
    has_slow = jnp.logical_and(slow_dev >= 0, slow_dev < rows_n)
    slow_up = jnp.logical_and(has_slow, odd == 0)
    slow_down = jnp.logical_and(has_slow, odd == 1)

    def z_copy(t, row):
        return remote(z.at[row, pl.ds(0, zn)], zhalo.at[t], z_send.at[t], z_recv.at[t],
                      {"sp": slow_dev, "sp2": sp2})

    def all_sum(layer, s1, s2, fold, ahead=lambda: None):
        s1 = jnp.sum(s1, axis=0, keepdims=True)
        s2 = jnp.sum(s2, axis=0, keepdims=True)
        both = jnp.concatenate([s1, s2], axis=0)
        if fold:
            half = both[:, :ca] + both[:, ca:]
            both = jnp.concatenate([half, half], axis=1)
        stat[layer, me] = both
        sends = [remote(stat.at[layer, me], stat.at[layer, me], st_send.at[layer, d], st_recv.at[layer, d], peer(d))
                 for d in range(1, n_dev)]
        for s in sends:
            s.start()
        ahead()
        for d in range(1, n_dev):
            src = (me + n_dev - d) % n_dev
            remote(stat.at[layer, src], stat.at[layer, src], st_send.at[layer, d], st_recv.at[layer, d], peer(d)).wait_recv()
        for s in sends:
            s.wait_send()
        total = stat[layer, 0]
        for k in range(1, n_dev):
            total = total + stat[layer, k]
        return total

    def affine(total, num, gamma, beta):
        mean = total[0:1] / num
        var = total[1:2] / num - mean * mean
        scale = gamma * lax.rsqrt(var + EPS)
        return scale, beta - mean * scale, jnp.zeros_like(beta)

    def group(n, q):
        return (0, n) if q is None else (((0,) + FRAC)[q] * n // 8, FRAC[q] * n // 8)

    def load_x_row(r):
        x_copy(r).wait()

        def blk(c, carry):
            for g in range(2):
                c0 = pl.multiple_of(c * 32 + g * 16, 16)
                for i in range(imgs):
                    stg[g, pl.ds(i * 17, 16), :] = xv[i, r, pl.ds(c0, 16), :].astype(F32)
            for g in range(2):
                base = pl.multiple_of((2 * c + g) * (8 * imgs), 8 * imgs)
                for k in range(16):
                    z[r, pl.ds(base + (k // 2) * imgs, imgs),
                      (k % 2) * ca:(k % 2 + 1) * ca] = stg[g, pl.ds(k, imgs, stride=17), :]
            return carry

        lax.fori_loop(0, cols // 32, blk, 0)

    def apply_bn(zz, aff):
        scale, shift, low = aff
        return jnp.maximum(zz * scale + shift, low)

    JN = 8

    def norm_a(r, p, aff):
        off = p * imgs if isinstance(p, int) else pl.multiple_of(p * imgs, JN * imgs)
        y = apply_bn(z[r, pl.ds(off, JN * imgs), :], aff).astype(BF16).reshape(JN, imgs, 2 * ca)
        y = jnp.stack([y[:, :, :ca], y[:, :, ca:]], axis=1).reshape(2 * JN, imgs, ca)
        act[r + 1, pl.ds(1 + 2 * p, 2 * JN)] = y

    def norm_row_a(r, aff, q=None):
        def blk(c, carry):
            norm_a(r, c * JN, aff)
            return carry
        lax.fori_loop(*group(pairs // JN, q), blk, 0)

    def norm_row_b(r, aff, q=None):
        def blk(c, carry):
            zz = z[r, pl.ds(pl.multiple_of(c * (JN * imgs), JN * imgs), JN * imgs), :]
            actb[r + 1, pl.ds(1 + c * JN, JN)] = apply_bn(zz, aff).astype(BF16).reshape(JN, imgs, cb)
            return carry
        lax.fori_loop(*group(cols_b // JN, q), blk, 0)

    def norm_col_a(aff):
        p = jnp.where(at_left, pairs - 1, 0)
        for r in range(rows):
            y = apply_bn(z[r, pl.ds(pl.multiple_of(p * imgs, imgs), imgs), :], aff).astype(BF16)
            cbuf_a[r] = jnp.where(at_left, y[:, ca:], y[:, :ca])

    def norm_col_b(aff):
        p = jnp.where(at_left, cols_b - 1, 0)
        for r in range(rows_b):
            cbuf_b[r] = apply_bn(z[r, pl.ds(pl.multiple_of(p * imgs, imgs), imgs), :], aff).astype(BF16)

    def put(r, c0, n_c, acc, s):
        off = c0 * imgs if isinstance(c0, int) else pl.multiple_of(c0 * imgs, 8 * imgs)
        z[r, pl.ds(off, n_c * imgs), :] = acc
        a3 = acc.reshape(n_c * imgs // 8, 8, acc.shape[-1])
        return s[0] + jnp.sum(a3, axis=0), s[1] + jnp.sum(a3 * a3, axis=0)

    JC = 16
    NC_A, NC_B = pairs // JC, cols_b // JC

    def conv_a(layer, r, c0, s, n=JC):
        parts = []
        for dy in range(3):
            v = act[r + dy, 2 * c0:2 * c0 + 2 * n + 2].reshape(n + 1, 2, imgs, ca)
            for c in range(4):
                parts.append(v[c // 2:c // 2 + n, c % 2].reshape(n * imgs, ca))
        acc = jnp.dot(jnp.concatenate(parts, axis=1), wp[layer], preferred_element_type=F32)
        return put(r, c0, n, acc, s)

    def conv_d(i, c0, s, n=JC):
        first, last = [], []
        for dy in range(3):
            v = act[2 * i + dy + 1, 2 * c0 + 1:2 * c0 + 2 * n + 2]
            a = v[:2 * n].reshape(n, 2, imgs, ca)
            b = v[1:].reshape(n, 2, imgs, ca)
            first += [a[:, 0].reshape(n * imgs, ca), a[:, 1].reshape(n * imgs, ca)]
            last.append(b[:, 1].reshape(n * imgs, ca))
        acc = jnp.dot(jnp.concatenate(first + last, axis=1), wdp[...], preferred_element_type=F32)
        return put(i, c0, n, acc, s)

    def conv_b(layer, r, c0, s, n=JC):
        parts = []
        for dy in range(3):
            for dx in range(3):
                parts.append(actb[r + dy, c0 + dx:c0 + dx + n].reshape(n * imgs, cb))
        acc = jnp.dot(jnp.concatenate(parts, axis=1), wbv[layer], preferred_element_type=F32)
        return put(r, c0, n, acc, s)

    def slow_parts(n_c):
        for q in range(NQ):
            lo, hi = group(n_c, q)
            yield q, [(lo, (hi - lo) // 2), ((lo + hi) // 2, (hi - lo) // 2)]

    zero_stat = lambda: (jnp.zeros((8, 256), F32), jnp.zeros((8, 256), F32))

    for c in early:
        c.wait()

    for layer in range(la):
        for dy in range(3):
            for c in range(4):
                k0 = (dy * 4 + c) * ca
                zero = jnp.zeros((ca, ca), BF16)
                wp[layer, k0:k0 + ca, :ca] = wa_ref[layer, dy, c] if c < 3 else zero
                wp[layer, k0:k0 + ca, ca:] = wa_ref[layer, dy, c - 1] if c > 0 else zero

    num_a = float(imgs * rows * cols * n_dev)
    num_b = float(imgs * rows_b * cols_b * n_dev)

    def dup(v):
        return jnp.concatenate([v, v], axis=1)

    ha = halo(act, cbuf_a, rows, cols)
    halves = ((0, range(0, 3)), (1, range(3, NQ)))

    def layer_a(layer, aff):
        norm_col_a(aff)
        norm_row_a(slow_row, aff, 0)
        send_corner(ha, is_slow)
        ha[2](cbuf_a).start()
        send_corner(ha, is_fast)
        produce_row(ha, is_slow, lambda q: norm_row_a(slow_row, aff, q) if q else None)
        produce_row(ha, is_fast, lambda q: norm_row_a(fast_row, aff, q))

        s = zero_stat()
        mid = [j * JC for j in range(NC_A // 4, NC_A - NC_A // 4)]
        outer = [j * JC for j in range(NC_A) if j * JC not in mid]
        inner = range(1, rows - 1)
        first = range(mid[0] - JN, mid[-1] + JC + 1, JN)
        rest = [(r, p) for r in inner for p in range(0, pairs, JN) if p not in first]
        ready = {r: [(r, p) for p in first] for r in inner}
        for pos, r in enumerate(inner):
            if pos == 0:
                start = sorted(ready[r] + ready[r + 1], key=lambda rp: rp[1])
                now = [start[:8], start[8:]]
                for rp in now[0]:
                    norm_a(*rp, aff)
            for u, c0 in enumerate(mid):
                if pos == 0 and u == 1:
                    for rp in now[1]:
                        norm_a(*rp, aff)
                s = conv_a(layer, r, c0, s)
                todo = ready.get(r + 2)
                if todo is None:
                    todo, left = rest, len(inner) - pos
                    take = -(-len(todo) // ((left - 1) * len(mid) + len(mid) - u))
                else:
                    take = -(-len(todo) // (len(mid) - u))
                for rp in todo[:take]:
                    norm_a(*rp, aff)
                del todo[:take]

        ha[5](cbuf_a).wait_recv()
        wait_row(ha, is_fast, True, range(NQ))
        for r in inner:
            for c0 in outer:
                s = conv_a(layer, r, c0, s)
        for j in range(NC_A):
            s = conv_a(layer, fast_row, j * JC, s)
        for part, pieces in halves:
            wait_row(ha, is_slow, part == 0, pieces)
            for j in range(part * NC_A // 2, (part + 1) * NC_A // 2):
                s = conv_a(layer, slow_row, j * JC, s)
        total = all_sum(layer, *s, True, lambda: pl.when(jnp.logical_and(slow_up, layer == la - 1))(
            lambda: z_copy(0, 0).start()))
        drain_row(ha, is_slow)
        drain_row(ha, is_fast)
        ha[2](cbuf_a).wait_send()
        return affine(total, num_a, dup(bna_ref[layer, 0:1]), dup(bna_ref[layer, 1:2]))

    load_x_row(slow_row)
    load_x_row(fast_row)
    lax.fori_loop(1, rows - 1, lambda r, c: (load_x_row(r), c)[1], 0)
    flat = jnp.zeros((1, 2 * ca), F32)
    aff = lax.fori_loop(0, la, layer_a, (flat + 1.0, flat, flat - jnp.inf))

    norm_col_a(aff)
    norm_row_a(0, aff, 0)

    @pl.when(sp2 == 1)
    def _():
        pl.when(has_up)(lambda: ha[1](0).start())
        ha[2](cbuf_a).start()

    fast_up = jnp.logical_and(has_up, odd == 1)
    fast_down = jnp.logical_and(has_down, odd == 0)
    for q in range(1, NQ):
        norm_row_a(0, aff, q)
        pl.when(has_up if q > 1 else fast_up)(lambda q=q: ha[0](0, q - 1).start())
    pl.when(has_up)(lambda: ha[0](0, NQ - 1).start())

    def inner_d(r, c):
        norm_row_a(r, aff)
        return c

    lax.fori_loop(1, rows, inner_d, 0)
    for c in w_copies:
        c.wait()

    pl.when(slow_up)(lambda: z_copy(0, 0).wait_send())
    s = zero_stat()
    for i in range(rows_b - 1):
        for c0 in range(0, cols_b - JC, JC):
            s = conv_d(i, c0, s)

    @pl.when(slow_down)
    def _():
        z_copy(0, 0).wait_recv()
        y = apply_bn(zhalo[0], aff).astype(BF16).reshape(zn // imgs, imgs, 2 * ca)
        y = jnp.stack([y[:, :, :ca], y[:, :, ca:]], axis=1).reshape(2 * zn // imgs, imgs, ca)
        act[rows + 1, 1:cols // 8 + 2] = y[:cols // 8 + 1]

    pl.when(sp2 == 0)(lambda: ha[5](cbuf_a).wait_recv())
    for i in range(rows_b - 1):
        for c0 in (cols_b - JC, cols_b - JC // 2):
            s = conv_d(i, c0, s, JC // 2)
    for q, chunks in slow_parts(cols_b):
        if q == 0:
            pl.when(jnp.logical_and(has_down, sp2 == 0))(lambda: ha[4](1).wait_recv())
        pl.when(has_down if q else fast_down)(lambda: ha[3](1, q).wait_recv())
        for c0, n in chunks:
            s = conv_d(rows_b - 1, c0, s, n)
    slow_b = odd * (rows_b - 1)
    total = all_sum(la, *s, False, lambda: pl.when(has_slow)(lambda: z_copy(1, slow_b).start()))

    pl.when(fast_up)(lambda: ha[0](0, 0).wait_send())

    @pl.when(has_up)
    def _():
        for q in range(1, NQ):
            ha[0](0, q).wait_send()
        pl.when(sp2 == 1)(lambda: ha[1](0).wait_send())

    @pl.when(sp2 == 1)
    def _():
        ha[2](cbuf_a).wait_send()

    aff = affine(total, num_b, bnd_ref[0:1], bnd_ref[1:2])

    hb = halo(actb, cbuf_b, rows_b, cols_b)
    fast_b = (rows_b - 1) - slow_b

    def layer_b(layer, aff):
        norm_col_b(aff)
        norm_row_b(slow_b, aff, 0)
        send_corner(hb, is_slow)
        hb[2](cbuf_b).start()
        send_corner(hb, is_fast)
        produce_row(hb, is_slow, lambda q: norm_row_b(slow_b, aff, q) if q else None, 1)
        produce_row(hb, is_fast, lambda q: norm_row_b(fast_b, aff, q))

        def inner(r, c):
            norm_row_b(r, aff)
            return c
        lax.fori_loop(1, rows_b - 1, inner, 0)
        s = zero_stat()
        for r in range(1, rows_b - 1):
            for c0 in range(JC, cols_b - JC, JC):
                s = conv_b(layer, r, c0, s)

        def first_piece(side):
            z_copy(1 + layer, slow_b).wait_send()
            z_copy(1 + layer, slow_b).wait_recv()
            y = apply_bn(zhalo[1 + layer], aff).astype(BF16).reshape(zn // imgs, imgs, cb)
            actb[(0, rows_b + 1)[side], 1:zn // imgs + 1] = y
        by_side(is_slow, first_piece)
        hb[5](cbuf_b).wait_recv()
        wait_row(hb, is_fast, True, range(NQ))
        for r in range(1, rows_b - 1):
            for c0 in (0, cols_b - JC):
                s = conv_b(layer, r, c0, s)
        for c0 in range(0, cols_b, JC):
            s = conv_b(layer, fast_b, c0, s)
        for q, chunks in slow_parts(cols_b):
            wait_row(hb, is_slow, q == 0, [q] if q else [])
            for c0, n in chunks:
                s = conv_b(layer, slow_b, c0, s, n)
        total = all_sum(la + 1 + layer, *s, False, lambda: pl.when(jnp.logical_and(has_slow, layer + 1 < lb))(
            lambda: z_copy(2 + layer, slow_b).start()))
        drain_row(hb, is_slow, 1)
        drain_row(hb, is_fast)
        hb[2](cbuf_b).wait_send()
        return affine(total, num_b, bnb_ref[layer, 0:1], bnb_ref[layer, 1:2])

    aff = lax.fori_loop(0, lb, layer_b, aff)

    def final_row(r, carry):
        def half_block(c0, g):
            for k in range(16):
                y = apply_bn(z[r, pl.ds(pl.multiple_of(c0 * imgs + k * imgs, imgs), imgs), :], aff)
                for h in range(2):
                    stg[g + h, pl.ds(k * 33, imgs), :] = y[:, h * 128:(h + 1) * 128]

        def turn(c0, g):
            for i in range(imgs):
                for h in range(2):
                    y_ref[i, r, pl.ds(c0, 16), h * 128:(h + 1) * 128] = stg[g + h, pl.ds(i, 16, stride=33), :].astype(BF16)

        def blk(c, carry):
            c0 = pl.multiple_of(c * 32, 32)
            half_block(c0, 0)
            half_block(c0 + 16, 2)
            turn(c0, 0)
            turn(pl.multiple_of(c0 + 16, 16), 2)
            return carry
        return lax.fori_loop(0, cols_b // 32, blk, carry)

    lax.fori_loop(0, rows_b, final_row, 0)


def solution(mesh):
    rows_n, cols_n = mesh.shape["sp"], mesh.shape["sp2"]

    def per_device(x, w_a, bn_a, w_down, bn_down, w_b, bn_b):
        imgs, rows, cols, ca = x.shape
        cb = w_down.shape[-1]
        la, lb = w_a.shape[0], w_b.shape[0]
        rows_b, cols_b = rows // 2, cols // 2
        dims = (imgs, rows, cols, ca, cb, la, lb, rows_n, cols_n)
        n_dev = rows_n * cols_n
        layers = la + 1 + lb
        vm = pl.BlockSpec(memory_space=pltpu.VMEM)
        hbm = pl.BlockSpec(memory_space=pl.ANY)
        dma = pltpu.SemaphoreType.DMA
        return pl.pallas_call(
            functools.partial(stack_kernel, dims),
            out_shape=pltpu.VMEM((imgs, rows_b, cols_b, cb), BF16),
            in_specs=[hbm] * 7,
            out_specs=vm,
            scratch_shapes=[
                pltpu.VMEM(w_a.shape, BF16),
                pltpu.VMEM(bn_a.shape, F32), pltpu.VMEM(bn_down.shape, F32), pltpu.VMEM(bn_b.shape, F32),
                pltpu.VMEM((imgs, rows, cols, ca), BF16),
                pltpu.VMEM((rows + 2, cols + 2, imgs, ca), BF16),
                pltpu.VMEM((rows_b + 2, cols_b + 2, imgs, cb), BF16),
                pltpu.VMEM((rows, cols // 2 * imgs, 2 * ca), F32),
                pltpu.VMEM((4, imgs * 17 + 16, 128), F32),
                pltpu.VMEM((la, 12 * ca, 2 * ca), BF16),
                pltpu.VMEM((9 * ca, cb), BF16),
                pltpu.VMEM((lb, 9 * cb, cb), BF16),
                pltpu.VMEM((rows, imgs, ca), BF16),
                pltpu.VMEM((rows_b, imgs, cb), BF16),
                pltpu.VMEM((layers, n_dev, 2, 256), F32),
                pltpu.VMEM((lb + 1, (cols_b // 8 + 1) * imgs, 256), F32),
                dma((rows,)), dma((14,)), dma((lb + 1,)), dma((lb + 1,)),
                dma((2, NQ)), dma((2, NQ)), dma((3,)), dma((3,)), dma((layers, n_dev)), dma((layers, n_dev)),
            ],
            compiler_params=pltpu.CompilerParams(
                collective_id=0, has_side_effects=True, vmem_limit_bytes=58_000_000),
            name="stack",
        )(x, w_a, bn_a, w_down, bn_down, w_b.reshape(lb, 9 * cb, cb), bn_b)

    tile_spec = P("dp", "sp", "sp2", None)
    return jax.shard_map(per_device, mesh=mesh, in_specs=(tile_spec, P(), P(), P(), P(), P(), P()),
                         out_specs=tile_spec, check_vma=False)
```
